32 devices in a mesh: grp: 4 (over y, x), sub: 8 (over z, core).
Axes of the slice: x: 2, y: 2, z: 4, core: 2. Of those that a mesh axis runs over, the one named last changes fastest.
Arguments:
- reg_disp: float32 [4, 8, 3, 384], P('grp', 'sub'), may hold values from -6 to 6
- reg_vel: float32 [4, 8, 3, 384], P('grp', 'sub'), may hold values from -0.6 to 0.6
- site_disp: float32 [4, 8, 3, 1536], P('grp', 'sub'), may hold values from -6 to 6
- site_vel: float32 [4, 8, 3, 1536], P('grp', 'sub'), may hold values from -0.6 to 0.6
- reg_nodes: int32 [4, 8, 10, 256], P('grp', 'sub'), may hold values from 0 to 383
- site_nodes: int32 [4, 8, 35, 128], P('grp', 'sub'), may hold values from 0 to 1535
- reg_coefs: float32 [4, 8, 3, 3, 4, 256], P('grp', 'sub'), may hold values from -1.5 to 6, as said below
- site_coefs: float32 [4, 8, 3, 3, 24, 128], P('grp', 'sub'), may hold values from -1.5 to 6, as said below
- reg_table: float32 [12, 10], replicated, may hold values from -2 to 2
- site_table: float32 [72, 35], replicated, may hold values from -1 to 1
- reg_minv: float32 [4, 8, 384], P('grp', 'sub'), may hold values from 0.003 to 0.015
- site_minv: float32 [4, 8, 1536], P('grp', 'sub'), may hold values from 0.003 to 0.015
- reg_send: int32 [4, 8, 2, 128], P('grp', 'sub'), may hold values from 0 to 383
- reg_recv: int32 [4, 8, 2, 128], P('grp', 'sub'), may hold values from 0 to 383
- site_send: int32 [4, 8, 2, 128], P('grp', 'sub'), may hold values from 0 to 1535
- site_recv: int32 [4, 8, 2, 128], P('grp', 'sub'), may hold values from 0 to 1535
- slot_fill: int32 [4, 8, 4], P('grp', 'sub'), may hold values from 1 to 128, 384 in all within a row
- layer_src: int32 [4, 8, 128], P('grp', 'sub'), may hold values from 0 to 383
- layer_fill: int32 [4, 8], P('grp', 'sub'), may hold values from 64 to 128, as said below
- layer_dst: int32 [4, 8, 3, 128], P('grp', 'sub'), may hold values from 0 to 1535
- layer_stiff: float32 [4, 8, 3, 128], P('grp', 'sub'), may hold values from 0.5 to 2
Outputs:
- reg_final: float32 [4, 8, 3, 384], P('grp', 'sub')
- site_final: float32 [4, 8, 3, 1536], P('grp', 'sub')
The draws below stay inside these ranges and needn't reach their ends.
Inputs may be any that keep to these rules, and one draw needn't show every extreme that they name: `slot_fill`: per partition the four entries count live slots toward the lower and higher neighbour, regional then site; they sum to 384. `layer_fill`: partition index 0 of every group fills all 128 slots. `reg_coefs`: each 3 x 3 tensor over the first two dimensions is symmetric positive definite. `site_coefs`: each 3 x 3 tensor over the first two dimensions is symmetric positive definite.
All inputs are finite; a program needn't handle non-finite values.
Results may differ from the reference program's by a relative error of at most 0.0003.
Values sent between devices are 32-bit elements; how exact they have to be, the bound alone decides.
No kernel may reach another device: no remote copies, remote signals or barrier semaphores. Data moves between devices by JAX's collectives and lax.ppermute only.
A program may use at most 64 MiB of HBM per device.

```python
import math
import jax
import jax.numpy as jnp
import numpy as np
from jax import lax

PR = 10
QR = 4
PS = 35
QS = 24
STEPS = 8
ES = 128
SLOTS = 128
DRM = 128
ER = 256
NR = 384
NS = 1536
N_GRP = 4
N_SUB = 8


def tensor_draw(key, quad_count, elem_count):
    first_key, second_key = jax.random.split(key)
    shape_diag = (N_GRP, N_SUB, 3, quad_count, elem_count)
    diagonal = jnp.exp(jax.random.uniform(first_key, shape_diag, jnp.float32, math.log(0.5), math.log(4.0)))
    off_diag = jax.random.uniform(second_key, (N_GRP, N_SUB, 3, 3, quad_count, elem_count), jnp.float32, -0.25, 0.25)
    off_diag = 0.5 * (off_diag + jnp.swapaxes(off_diag, 2, 3))
    identity = jnp.eye(3, dtype=jnp.float32)[:, :, None, None]
    off_diag = off_diag * (1.0 - identity)
    root_scale = jnp.sqrt(diagonal)
    return root_scale[:, :, :, None] * root_scale[:, :, None, :] * (identity + off_diag)


def draw_reg_coefs(key, part):
    return tensor_draw(jax.random.fold_in(key, 11), QR, ER)


def draw_site_coefs(key, part):
    return tensor_draw(jax.random.fold_in(key, 23), QS, ES)


def draw_layer_fill(key, part):
    counts = jax.random.randint(jax.random.fold_in(key, 37), (N_GRP, N_SUB), DRM // 2, DRM + 1, dtype=jnp.int32)
    return counts.at[:, 0].set(DRM)


def touch_ends(array, rng, low, high):
    place = [jax.random.randint(jax.random.fold_in(rng, axis), (), 0, length) for axis, length in enumerate(array.shape)]
    main_axis = array.shape.index(max(array.shape))
    next_to = place[:main_axis] + [(place[main_axis] + 1) % array.shape[main_axis]] + place[main_axis + 1:]
    return array.at[tuple(place)].set(low).at[tuple(next_to)].set(high)


def block_scale(key, shape, shards, low, high):
    def one(dim, blocks):
        heights = jax.random.uniform(jax.random.fold_in(jax.random.fold_in(key, 6), dim), (blocks,), jnp.float32, low / len(shards), high / len(shards))
        return jnp.repeat(jnp.exp(heights), shape[dim] // blocks).reshape((-1,) + (1,) * (len(shape) - dim - 1))

    loudness = one(*shards[0])
    for cut in shards[1:]:
        loudness = loudness * one(*cut)
    return loudness


def length_profile(count, total, bound, slope):
    weights = [(1 << 20) // math.isqrt(grade ** slope) + 1 for grade in range(2, count + 1)]
    surplus, given = total - bound - (count - 1), [1] * (count - 1)
    while surplus > 0:
        free = [i for i in range(count - 1) if given[i] < bound]
        whole, budget = sum([weights[i] for i in free]), surplus
        for i in free:
            more = min(bound - given[i], max(1, budget * weights[i] // whole), surplus)
            given[i] = given[i] + more
            surplus = surplus - more
    return np.array([bound] + given)


def ragged_sizes(stream_key, amount, total, limit, lean):
    if amount == 2:
        one = jax.random.randint(stream_key, (), max(1, total - limit), min(limit, total - 1) + 1)
        return jnp.stack([one, total - one])
    tallies = jnp.asarray(length_profile(amount, total, limit, lean), jnp.int32)
    couples = (amount - 1) // 2
    donor, sink = tallies[1:1 + 2 * couples:2], tallies[2:2 + 2 * couples:2]
    margin = jnp.minimum(donor - 1, limit - sink)
    passed = jax.random.randint(jax.random.fold_in(stream_key, 1), (couples,), 0, 1 << 20) % (margin + 1)
    tallies = tallies.at[1:1 + 2 * couples:2].set(donor - passed).at[2:2 + 2 * couples:2].set(sink + passed)
    return tallies[jax.random.permutation(jax.random.fold_in(stream_key, 2), amount)]


def scatter_about(rng, shape, spread, bound, shards=(), held_as=jnp.bfloat16):
    entries = jax.random.normal(rng, shape, jnp.float32) * spread
    if len(shards) > 0:
        entries = block_scale(rng, shape, shards, -0.22, 0.18) * entries
    return jnp.clip(entries, min=-bound, max=bound).astype(held_as)


def setup_inputs(seed: int = 0) -> dict:
    key_list = jax.random.split(jax.random.key(seed), 22)
    reg_disp = scatter_about(key_list[0], (N_GRP, N_SUB, 3, NR), 1.0, 6.0, ((0, 4), (1, 8)), jnp.float32)
    reg_vel = scatter_about(key_list[1], (N_GRP, N_SUB, 3, NR), 0.1, 0.6, ((0, 4), (1, 8)), jnp.float32)
    site_disp = scatter_about(key_list[2], (N_GRP, N_SUB, 3, NS), 1.0, 6.0, ((0, 4), (1, 8)), jnp.float32)
    site_vel = scatter_about(key_list[3], (N_GRP, N_SUB, 3, NS), 0.1, 0.6, ((0, 4), (1, 8)), jnp.float32)
    reg_nodes = touch_ends(jax.random.randint(key_list[4], (N_GRP, N_SUB, PR, ER), 0, NR), jax.random.fold_in(key_list[4], 1), 0, NR - 1).astype(jnp.int32)
    site_nodes = touch_ends(jax.random.randint(key_list[5], (N_GRP, N_SUB, PS, ES), 0, NS), jax.random.fold_in(key_list[5], 1), 0, NS - 1).astype(jnp.int32)
    reg_coefs = draw_reg_coefs(jax.random.fold_in(key_list[21], 71), 0)
    site_coefs = draw_site_coefs(jax.random.fold_in(key_list[21], 71), 0)
    reg_table = scatter_about(key_list[8], (3 * QR, PR), PR ** -0.5, 2.0, (), jnp.float32)
    site_table = scatter_about(key_list[9], (3 * QS, PS), PS ** -0.5, 1.0, (), jnp.float32)
    reg_minv = jnp.clip(jnp.exp(math.log(0.015) - 1.60943788 * jax.random.uniform(key_list[10], (N_GRP, N_SUB, NR), jnp.float32) ** block_scale(key_list[10], (N_GRP, N_SUB, NR), ((0, 4), (1, 8)), -0.2, 0.2)), 0.003, 0.015)
    site_minv = jnp.clip(jnp.exp(math.log(0.015) - 1.60943788 * jax.random.uniform(key_list[11], (N_GRP, N_SUB, NS), jnp.float32) ** block_scale(key_list[11], (N_GRP, N_SUB, NS), ((0, 4), (1, 8)), -0.2, 0.2)), 0.003, 0.015)
    reg_send = touch_ends(jax.random.randint(key_list[12], (N_GRP, N_SUB, 2, SLOTS), 0, NR), jax.random.fold_in(key_list[12], 1), 0, NR - 1).astype(jnp.int32)
    reg_recv = touch_ends(jax.random.randint(key_list[13], (N_GRP, N_SUB, 2, SLOTS), 0, NR), jax.random.fold_in(key_list[13], 1), 0, NR - 1).astype(jnp.int32)
    site_send = touch_ends(jax.random.randint(key_list[14], (N_GRP, N_SUB, 2, SLOTS), 0, NS), jax.random.fold_in(key_list[14], 1), 0, NS - 1).astype(jnp.int32)
    site_recv = touch_ends(jax.random.randint(key_list[15], (N_GRP, N_SUB, 2, SLOTS), 0, NS), jax.random.fold_in(key_list[15], 1), 0, NS - 1).astype(jnp.int32)
    slot_fill = jax.vmap(lambda own: ragged_sizes(own, 4, 3 * SLOTS, SLOTS, 0))(jax.random.split(key_list[16], N_GRP * N_SUB)).reshape((N_GRP, N_SUB, 4)).astype(jnp.int32)
    layer_src = touch_ends(jax.random.randint(key_list[17], (N_GRP, N_SUB, DRM), 0, NR), jax.random.fold_in(key_list[17], 1), 0, NR - 1).astype(jnp.int32)
    layer_fill = draw_layer_fill(jax.random.fold_in(key_list[21], 71), 0)
    layer_dst = touch_ends(jax.random.randint(key_list[19], (N_GRP, N_SUB, 3, DRM), 0, NS), jax.random.fold_in(key_list[19], 1), 0, NS - 1).astype(jnp.int32)
    layer_stiff = jnp.clip(jnp.exp(math.log(2.0) - 1.3862944 * jax.random.uniform(key_list[20], (N_GRP, N_SUB, 3, DRM), jnp.float32) ** block_scale(key_list[20], (N_GRP, N_SUB, 3, DRM), ((0, 4), (1, 8)), -0.2, 0.2)), 0.5, 2.0)
    return {"reg_disp": reg_disp, "reg_vel": reg_vel, "site_disp": site_disp, "site_vel": site_vel, "reg_nodes": reg_nodes, "site_nodes": site_nodes, "reg_coefs": reg_coefs, "site_coefs": site_coefs, "reg_table": reg_table, "site_table": site_table, "reg_minv": reg_minv, "site_minv": site_minv, "reg_send": reg_send, "reg_recv": reg_recv, "site_send": site_send, "site_recv": site_recv, "slot_fill": slot_fill, "layer_src": layer_src, "layer_fill": layer_fill, "layer_dst": layer_dst, "layer_stiff": layer_stiff}


PRECISE = lax.Precision.HIGHEST


def stiff_force(displaced, element_nodes, coef_block, deriv_table):
    quad_count = coef_block.shape[2]
    node_count = element_nodes.shape[0]
    elem_count = element_nodes.shape[1]
    flat_nodes = element_nodes.reshape(-1)
    gathered = jnp.take(displaced, flat_nodes, axis=1).reshape(3, node_count, elem_count)
    gradient = jnp.einsum("kp,cpe->cke", deriv_table, gathered, precision=PRECISE)
    pieces = [gradient[:, b * quad_count:(b + 1) * quad_count] for b in range(3)]
    flux_rows = [coef_block[a, 0][None] * pieces[0] + coef_block[a, 1][None] * pieces[1] + coef_block[a, 2][None] * pieces[2] for a in range(3)]
    flux_terms = jnp.concatenate(flux_rows, axis=1)
    element_terms = jnp.einsum("kp,cke->cpe", deriv_table, flux_terms, precision=PRECISE)
    return -jnp.zeros_like(displaced).at[:, flat_nodes].add(element_terms.reshape(3, -1))


def pack_slots(forces, send_map, fill_pair):
    picked = jnp.take(forces, send_map, axis=1)
    live_slots = jnp.arange(send_map.shape[1], dtype=jnp.int32)[None, :] < fill_pair[:, None]
    return jnp.where(live_slots[:, None, :], jnp.transpose(picked, (1, 0, 2)), 0.0)


def take_slots(forces, recv_map, from_lower, from_upper):
    return forces.at[:, recv_map[0]].add(from_lower).at[:, recv_map[1]].add(from_upper)


def pack_layer(displaced, layer_src, layer_fill):
    picked = jnp.take(displaced, layer_src, axis=1)
    live_slots = jnp.arange(layer_src.shape[0], dtype=jnp.int32) < layer_fill
    return jnp.where(live_slots[None, :], picked, 0.0)


def add_layer(forces, layer_dst, layer_stiff, layer_block):
    for source in range(3):
        forces = forces.at[:, layer_dst[source]].add(layer_stiff[source][None, :] * layer_block[source])
    return forces


def neighbour_terms(send_rows, group_rows):
    shaped = send_rows.reshape((group_rows, N_SUB) + send_rows.shape[1:])
    blank_rows = jnp.zeros_like(shaped[:, :1, 0])
    from_lower = jnp.concatenate([blank_rows, shaped[:, :-1, 1]], axis=1)
    from_upper = jnp.concatenate([shaped[:, 1:, 0], blank_rows], axis=1)
    width = send_rows.shape[-1]
    return from_lower.reshape(-1, 3, width), from_upper.reshape(-1, 3, width)


def reference(reg_disp, reg_vel, site_disp, site_vel, reg_nodes, site_nodes, reg_coefs, site_coefs, reg_table, site_table, reg_minv, site_minv, reg_send, reg_recv, site_send, site_recv, slot_fill, layer_src, layer_fill, layer_dst, layer_stiff):
    site_groups = N_GRP // 4
    reg_groups = 3 * site_groups

    def regional(stacked):
        return stacked[:reg_groups].reshape((reg_groups * N_SUB,) + stacked.shape[2:])

    def sitewise(stacked):
        return stacked[reg_groups:].reshape((site_groups * N_SUB,) + stacked.shape[2:])

    reg_now = regional(reg_disp)
    reg_prev = reg_now - regional(reg_vel)
    r_nodes, r_coefs, r_minv = regional(reg_nodes), regional(reg_coefs), regional(reg_minv)
    r_send, r_recv, r_fill = regional(reg_send), regional(reg_recv), regional(slot_fill)[:, 0:2]
    r_src, r_layer_fill = regional(layer_src), regional(layer_fill)
    layers = []
    for step_no in range(STEPS):
        forces = lax.map(lambda device_items: stiff_force(device_items[0], device_items[1], device_items[2], reg_table), (reg_now, r_nodes, r_coefs))
        send_rows = jax.vmap(pack_slots)(forces, r_send, r_fill)
        from_lower, from_upper = neighbour_terms(send_rows, reg_groups)
        forces = jax.vmap(take_slots)(forces, r_recv, from_lower, from_upper)
        reg_next = 2.0 * reg_now - reg_prev + r_minv[:, None, :] * forces
        reg_prev, reg_now = reg_now, reg_next
        layers.append(jax.vmap(pack_layer)(reg_now, r_src, r_layer_fill))

    site_now = sitewise(site_disp)
    site_prev = site_now - sitewise(site_vel)
    s_nodes, s_coefs, s_minv = sitewise(site_nodes), sitewise(site_coefs), sitewise(site_minv)
    s_send, s_recv, s_fill = sitewise(site_send), sitewise(site_recv), sitewise(slot_fill)[:, 2:4]
    s_dst, s_stiff = sitewise(layer_dst), sitewise(layer_stiff)
    for step_no in range(STEPS):
        forces = lax.map(lambda device_items: stiff_force(device_items[0], device_items[1], device_items[2], site_table), (site_now, s_nodes, s_coefs))
        send_rows = jax.vmap(pack_slots)(forces, s_send, s_fill)
        from_lower, from_upper = neighbour_terms(send_rows, site_groups)
        forces = jax.vmap(take_slots)(forces, s_recv, from_lower, from_upper)
        layer_block = layers[step_no].reshape(3, site_groups, N_SUB, 3, -1)
        layer_block = jnp.transpose(layer_block, (1, 2, 0, 3, 4)).reshape(site_groups * N_SUB, 3, 3, -1)
        forces = jax.vmap(add_layer)(forces, s_dst, s_stiff, layer_block)
        site_next = 2.0 * site_now - site_prev + s_minv[:, None, :] * forces
        site_prev, site_now = site_now, site_next

    reg_final = jnp.concatenate([reg_now.reshape((reg_groups, N_SUB) + reg_now.shape[1:]),
                                 jnp.zeros((site_groups, N_SUB) + reg_now.shape[1:], jnp.float32)], axis=0)
    site_final = jnp.concatenate([jnp.zeros((reg_groups, N_SUB) + site_now.shape[1:], jnp.float32),
                                  site_now.reshape((site_groups, N_SUB) + site_now.shape[1:])], axis=0)
    return reg_final, site_final
```

```python
import functools

import jax
import jax.numpy as jnp
from jax import lax
from jax.experimental import pallas as pl
from jax.experimental.pallas import tpu as pltpu
from jax.sharding import PartitionSpec as P

STEPS = 8
UNROLL = 4
LANES = 128
F32 = jnp.float32
BF16 = jnp.bfloat16
PAIRS = ((0, 0), (0, 1), (0, 2), (1, 1), (1, 2), (2, 2))
PAIR_OF = {**{ab: i for i, ab in enumerate(PAIRS)}, **{ab[::-1]: i for i, ab in enumerate(PAIRS)}}


def up_to(value, unit):
    return -(-value // unit) * unit


class Kind:
    def __init__(self, nodes, coefs, disp, slots, sources):
        self.points, self.elems = nodes.shape[-2:]
        self.quads = coefs.shape[-2]
        self.count = disp.shape[-1]
        self.blocks = self.count // LANES
        self.cuts = self.elems // LANES
        self.points_pad = up_to(self.points, 8)
        self.quads_pad = up_to(self.quads, 8)
        self.blocks_pad = up_to(self.blocks, 2)
        self.depth_in = up_to(3 * self.points_pad, 16)
        self.depth_out = up_to(9 * self.quads_pad, 16)
        self.chunks = self.points * self.cuts
        self.sources = sources
        self.tiles = up_to(self.chunks, 4) // 4
        self.extra = 2 + sources
        self.extra_tiles = up_to(self.extra, 4) // 4
        self.slots = slots
        row = 0
        for name, rows in (
            ("coefs", 6 * self.quads * self.cuts),
            ("nodes", self.points * self.cuts),
            ("disp", 3 * self.blocks),
            ("vel", 3 * self.blocks),
            ("minv", self.blocks),
            ("send", 2),
            ("recv", 2),
            ("layer", 2 * sources if sources else 1),
        ):
            setattr(self, "at_" + name, row)
            row += rows
        self.rows = up_to(row, 8)


def pack_kind(kind, out, disp, vel, nodes, coefs, minv, send, recv, fill, layer):
    for pair, (a, b) in enumerate(PAIRS):
        for cut in range(kind.cuts):
            at = kind.at_coefs + (pair * kind.cuts + cut) * kind.quads
            out[at : at + kind.quads, :] = coefs[0, 0, a, b, :, cut * LANES : (cut + 1) * LANES]
    for cut in range(kind.cuts):
        at = kind.at_nodes + cut * kind.points
        out[at : at + kind.points, :] = nodes[0, 0, :, cut * LANES : (cut + 1) * LANES].astype(F32)
    for block in range(kind.blocks):
        lanes = slice(block * LANES, (block + 1) * LANES)
        out[kind.at_disp + 3 * block : kind.at_disp + 3 * block + 3, :] = disp[0, 0, :, lanes]
        out[kind.at_vel + 3 * block : kind.at_vel + 3 * block + 3, :] = vel[0, 0, :, lanes]
        out[kind.at_minv + block : kind.at_minv + block + 1, :] = minv[0, 0:1, lanes]
    lane = lax.broadcasted_iota(jnp.int32, (1, LANES), 1)
    for side in range(2):
        live = lane < fill[side]
        row = send[0, 0, side : side + 1, :]
        out[kind.at_send + side : kind.at_send + side + 1, :] = jnp.where(live, row, -1).astype(F32)
    out[kind.at_recv : kind.at_recv + 2, :] = recv[0, 0].astype(F32)
    if kind.sources:
        layer_dst, layer_stiff = layer
        m = kind.sources
        out[kind.at_layer : kind.at_layer + m, :] = layer_dst[0, 0].astype(F32)
        out[kind.at_layer + m : kind.at_layer + 2 * m, :] = layer_stiff[0, 0]
    else:
        layer_src, layer_fill = layer
        live = lane < layer_fill
        row = layer_src[0, 0:1, :]
        out[kind.at_layer : kind.at_layer + 1, :] = jnp.where(live, row, -1).astype(F32)


def split_index(value):
    index = value.astype(jnp.int32)
    return index & (LANES - 1), index >> 7


def high_part(value):
    return value.astype(BF16).astype(F32)


def simulate(kind, width, unroll, buf, lhs_in, lhs_out, layers, emit, s):
    points, cuts, blocks = kind.points, kind.cuts, kind.blocks
    quads_pad = kind.quads_pad
    half_rows = 8 * kind.blocks_pad
    row8 = lax.broadcasted_iota(jnp.int32, (8, LANES), 0)
    low_half = row8 < 4
    row16 = lax.broadcasted_iota(jnp.int32, (16, LANES), 0)
    block_ids = [
        jnp.where(row16 < 8, 2 * j, 2 * j + 1).astype(F32).astype(BF16)
        for j in range(kind.blocks_pad // 2)
    ]
    zero16 = jnp.zeros((16, LANES), BF16)
    zero8 = jnp.zeros((8, LANES), F32)
    lane_ids = lax.broadcasted_iota(jnp.int32, (LANES, LANES), 1)
    main_rows = kind.tiles * 256

    def onehot(q, chunk_no, base_row, columns, at):
        hit = columns[:, at : at + 1] == lane_ids
        tile, half, part = chunk_no // 4, (chunk_no // 2) % 2, chunk_no % 2
        rows = pl.ds(base_row + tile * 256 + part * LANES, LANES)
        s.onehot[q, rows, half * LANES : (half + 1) * LANES] = jnp.where(hit, 1.0, 0.0).astype(BF16)

    def hold_block(q, chunk_no, hi_row):
        wide = jnp.broadcast_to(hi_row.astype(F32), (16, LANES))
        s.block_of[q, chunk_no] = wide.astype(BF16)

    def columns_of(rows):
        count = rows.shape[0]
        if count < LANES:
            rows = jnp.concatenate([rows, jnp.zeros((LANES - count, LANES), F32)], axis=0)
        return jnp.transpose(rows).astype(jnp.int32)

    def setup(q, _):
        for pair in range(6):
            for cut in range(cuts):
                at = kind.at_coefs + (pair * cuts + cut) * kind.quads
                lanes = slice(cut * LANES, (cut + 1) * LANES)
                if kind.quads_pad > kind.quads:
                    s.coefs[q, pair, :, lanes] = jnp.zeros((quads_pad, LANES), F32)
                s.coefs[q, pair, 0 : kind.quads, lanes] = buf[q, at : at + kind.quads, :]
        for cut in range(cuts):
            at = kind.at_nodes + cut * points
            value = buf[q, at : at + points, :]
            lo, hi = split_index(value)
            if kind.points_pad > points:
                s.lo[q, cut] = jnp.zeros((kind.points_pad, LANES), jnp.int32)
                s.hi[q, cut] = jnp.zeros((kind.points_pad, LANES), jnp.int32)
            s.lo[q, cut, 0:points, :] = lo
            s.hi[q, cut, 0:points, :] = hi
            columns = columns_of(lo.astype(F32))
            for p in range(points):
                onehot(q, cut * points + p, 0, columns, p)
                hold_block(q, cut * points + p, hi[p : p + 1, :])
        for chunk in range(kind.chunks, 4 * kind.tiles):
            columns = jnp.zeros((LANES, 1), jnp.int32)
            onehot(q, chunk, 0, columns, 0)
            hold_block(q, chunk, jnp.zeros((1, LANES), jnp.int32))
        extra = [buf[q, kind.at_recv : kind.at_recv + 2, :]]
        if kind.sources:
            extra.append(buf[q, kind.at_layer : kind.at_layer + kind.sources, :])
        extra.append(jnp.zeros((4 * kind.extra_tiles - kind.extra, LANES), F32))
        lo, hi = split_index(jnp.concatenate([e for e in extra if e.shape[0]], axis=0))
        columns = columns_of(lo.astype(F32))
        for chunk in range(4 * kind.extra_tiles):
            onehot(q, chunk, main_rows, columns, chunk)
            hold_block(q, 4 * kind.tiles + chunk, hi[chunk : chunk + 1, :])
        send_rows = [
            jnp.broadcast_to(buf[q, kind.at_send + side : kind.at_send + side + 1, :], (4, LANES))
            for side in range(2)
        ]
        s.send_lo[q], s.send_hi[q] = split_index(jnp.concatenate(send_rows, axis=0))
        if not kind.sources:
            row = buf[q, kind.at_layer : kind.at_layer + 1, :]
            s.layer_lo[q], s.layer_hi[q] = split_index(jnp.broadcast_to(row, (8, LANES)))
        for block in range(blocks):
            at = kind.at_disp + 3 * block
            now = buf[q, at : at + 3, :]
            at = kind.at_vel + 3 * block
            before = now - buf[q, at : at + 3, :]
            for ref, value in ((s.now, now), (s.before, before)):
                ref[q, block] = zero8
                ref[q, block, 0:3, :] = value
                ref[q, block, 4:7, :] = value
        return 0

    lax.fori_loop(0, width, setup, 0)
    for lane in range(unroll):
        s.parts[lane] = jnp.zeros(s.parts.shape[1:], F32)
        s.spread[lane] = jnp.zeros(s.spread.shape[1:], BF16)
        s.spread_extra[lane] = jnp.zeros(s.spread_extra.shape[1:], BF16)
    s.sends[0] = zero8
    s.sends[width + 1] = zero8

    def place(spread, lane, q, chunk_no, block_at, value8):
        doubled = jnp.concatenate([value8, value8], axis=0).astype(BF16)
        held = s.block_of[q, block_at]
        tile, half, part = chunk_no // 4, (chunk_no // 2) % 2, chunk_no % 2
        lanes = slice(tile * 256 + part * LANES, tile * 256 + (part + 1) * LANES)
        for j, ids in enumerate(block_ids):
            at = half * half_rows + 16 * j
            spread[lane, at : at + 16, lanes] = jnp.where(held == ids, doubled, zero16)

    def fold(total, block):
        rows = slice(block * 8, block * 8 + 8)
        other = slice(half_rows + block * 8, half_rows + block * 8 + 8)
        value = total[rows, 0:LANES] + total[other, LANES : 2 * LANES]
        return value + pltpu.roll(value, 4, 0)

    def pick(source, q, lo, hi):
        value = zero8
        for block in range(blocks):
            found = jnp.take_along_axis(source(block), lo, axis=1, mode="promise_in_bounds")
            value = jnp.where(hi == block, found, value)
        return value

    def force(q, lane):
        stacked = []
        picked = {}
        for cut in range(cuts):
            lo = s.lo[q, cut]
            hi = s.hi[q, cut]
            values = [jnp.zeros((kind.points_pad, LANES), F32)] * 3
            for block in range(blocks):
                here = hi == block
                for c in range(3):
                    row = jnp.broadcast_to(
                        s.now[q, block, c : c + 1, :], (kind.points_pad, LANES)
                    )
                    found = jnp.take_along_axis(row, lo, axis=1, mode="promise_in_bounds")
                    values[c] = jnp.where(here, found, values[c])
            for c in range(3):
                picked[c, cut] = values[c]
        order = [(c, cut) for c in range(3) for cut in range(cuts)]
        for key in order:
            high = high_part(picked[key])
            rows = [high, high, picked[key] - high]
            pad = kind.depth_in - 3 * kind.points_pad
            if pad:
                rows.append(jnp.zeros((pad, LANES), F32))
            stacked.append(jnp.concatenate(rows, axis=0).astype(BF16))
        grad = jnp.dot(
            lhs_in[...], jnp.concatenate(stacked, axis=1), preferred_element_type=F32
        )
        stacked = []
        for number, (c, cut) in enumerate(order):
            lanes = slice(number * LANES, (number + 1) * LANES)
            cut_lanes = slice(cut * LANES, (cut + 1) * LANES)
            pieces = [grad[b * quads_pad : (b + 1) * quads_pad, lanes] for b in range(3)]
            coef = [s.coefs[q, pair, :, cut_lanes] for pair in range(6)]
            flux = jnp.concatenate(
                [
                    coef[PAIR_OF[a, 0]] * pieces[0]
                    + coef[PAIR_OF[a, 1]] * pieces[1]
                    + coef[PAIR_OF[a, 2]] * pieces[2]
                    for a in range(3)
                ],
                axis=0,
            )
            high = high_part(flux)
            rows = [high, high, flux - high]
            pad = kind.depth_out - 9 * quads_pad
            if pad:
                rows.append(jnp.zeros((pad, LANES), F32))
            stacked.append(jnp.concatenate(rows, axis=0).astype(BF16))
        elem = jnp.dot(
            lhs_out[...], jnp.concatenate(stacked, axis=1), preferred_element_type=F32
        )
        for number, (c, cut) in enumerate(order):
            value = elem[:, number * LANES : (number + 1) * LANES]
            high = high_part(value)
            size = kind.points_pad
            s.parts[lane, cut, c * size : (c + 1) * size, :] = high
            s.parts[lane, cut, (c + 4) * size : (c + 5) * size, :] = value - high
        for cut in range(cuts):
            for p in range(points):
                value8 = s.parts[lane, cut, pl.ds(p, 8, stride=kind.points_pad), :]
                chunk = cut * points + p
                place(s.spread, lane, q, chunk, chunk, value8)
        total = jnp.dot(
            s.spread[lane], s.onehot[q, 0:main_rows, :], preferred_element_type=F32
        )
        folded = [fold(total, block) for block in range(blocks)]
        for block in range(blocks):
            s.force[q, block] = folded[block]
        s.sends[q + 1] = pick(lambda block: folded[block], q, s.send_lo[q], s.send_hi[q])

    def split8(value):
        high = high_part(value)
        return jnp.where(low_half, high, value - high)

    def update(q, lane, step):
        lower = s.sends[q]
        upper = s.sends[q + 2]
        values = [
            jnp.where(low_half, pltpu.roll(lower, 4, 0), lower),
            jnp.where(low_half, upper, pltpu.roll(upper, 4, 0)),
        ]
        for m in range(kind.sources):
            four = layers[m][step, q]
            at = kind.at_layer + kind.sources + m
            values.append(jnp.concatenate([four, four], axis=0) * buf[q, at : at + 1, :])
        for number, value in enumerate(values):
            place(s.spread_extra, lane, q, number, 4 * kind.tiles + number, split8(value))
        total = jnp.dot(
            s.spread_extra[lane],
            s.onehot[q, main_rows : main_rows + 256 * kind.extra_tiles, :],
            preferred_element_type=F32,
        )
        after = []
        for block in range(blocks):
            now = s.now[q, block]
            scale = buf[q, kind.at_minv + block : kind.at_minv + block + 1, :]
            whole = s.force[q, block] + fold(total, block)
            value = 2.0 * now - s.before[q, block] + scale * whole
            s.before[q, block] = now
            s.now[q, block] = value
            after.append(value)
        if emit is not None:
            picked = pick(lambda block: after[block], q, s.layer_lo[q], s.layer_hi[q])
            emit[step, q] = picked[0:4]

    def one_step(step, _):
        def forces(group, _):
            for lane in range(unroll):
                force(group * unroll + lane, lane)
            return 0

        def updates(group, _):
            for lane in range(unroll):
                update(group * unroll + lane, lane, step)
            return 0

        lax.fori_loop(0, width // unroll, forces, 0)
        lax.fori_loop(0, width // unroll, updates, 0)
        return 0

    lax.fori_loop(0, STEPS, one_step, 0)


SCRATCH = (
    "onehot", "block_of", "coefs", "lo", "hi", "send_lo", "send_hi", "layer_lo", "layer_hi",
    "now", "before", "force", "sends", "parts", "spread", "spread_extra",
)


def scratch_of(kind, width, unroll):
    tiles = kind.tiles + kind.extra_tiles
    rows = 16 * kind.blocks_pad
    return [
        pltpu.VMEM((width, tiles * 256, 256), BF16),
        pltpu.VMEM((width, 4 * tiles, 16, LANES), BF16),
        pltpu.VMEM((width, 6, kind.quads_pad, kind.elems), F32),
        pltpu.VMEM((width, kind.cuts, kind.points_pad, LANES), jnp.int32),
        pltpu.VMEM((width, kind.cuts, kind.points_pad, LANES), jnp.int32),
        pltpu.VMEM((width, 8, LANES), jnp.int32),
        pltpu.VMEM((width, 8, LANES), jnp.int32),
        pltpu.VMEM((width, 8, LANES), jnp.int32),
        pltpu.VMEM((width, 8, LANES), jnp.int32),
        pltpu.VMEM((width, kind.blocks, 8, LANES), F32),
        pltpu.VMEM((width, kind.blocks, 8, LANES), F32),
        pltpu.VMEM((width, kind.blocks, 8, LANES), F32),
        pltpu.VMEM((width + 2, 8, LANES), F32),
        pltpu.VMEM((unroll, kind.cuts, 8 * kind.points_pad, LANES), F32),
        pltpu.VMEM((unroll, rows, kind.tiles * 256), BF16),
        pltpu.VMEM((unroll, rows, kind.extra_tiles * 256), BF16),
    ]


class Refs:
    pass


def window_base(index, count, width):
    return jnp.clip(index - STEPS, 0, count - width)


def sim_kernel(kind, width, unroll, groups, offsets, has_layers, *refs):
    sub = lax.axis_index("sub")
    count = lax.axis_size("sub")
    chips = count // 2
    n_bufs = 2 * len(offsets)
    bufs, refs = refs[:n_bufs], refs[n_bufs:]
    lhs_in, lhs_out, refs = refs[0], refs[1], refs[2:]
    layers = None
    if has_layers:
        layers, refs = refs[: kind.sources], refs[kind.sources :]
    final, refs = refs[0], refs[1:]
    emit = None
    if not has_layers:
        emit, refs = refs[0], refs[1:]
    buf, sem, refs = refs[0], refs[1], refs[2:]
    s = Refs()
    for name, ref in zip(SCRATCH, refs, strict=True):
        setattr(s, name, ref)
    grp = lax.axis_index("grp")
    low, high = groups
    mine = jnp.logical_and(grp >= low, grp < high)
    base = window_base(sub, count, width)

    @pl.when(mine)
    def _():
        if width < count:
            buf[...] = jnp.zeros(buf.shape, F32)
        copies = []
        for number, offset in enumerate(offsets):
            for other in range(2):
                chip = lax.rem(sub // 2 - offset + chips, chips)
                core = lax.rem(sub, 2)
                slot = chip * 2 + (core if other == 0 else 1 - core) - base
                at = 2 * number + other
                inside = jnp.logical_and(slot >= 0, slot < width)
                slot = jnp.clip(slot, 0, width - 1)
                copy = pltpu.make_async_copy(bufs[at], buf.at[slot], sem.at[at])
                copies.append((inside, copy))
        for phase in ("start", "wait"):
            for inside, copy in copies:
                if width < count:
                    pl.when(inside)(getattr(copy, phase))
                else:
                    getattr(copy, phase)()
        simulate(kind, width, unroll, buf, lhs_in, lhs_out, layers, emit, s)
        for block in range(kind.blocks):
            final[0, 0, :, block * LANES : (block + 1) * LANES] = s.now[sub - base, block, 0:3, :]

    @pl.when(jnp.logical_not(mine))
    def _():
        final[...] = jnp.zeros(final.shape, F32)


def run_sim(kind, width, unroll, groups, offsets, bufs, tables, layers):
    has_layers = layers is not None
    out_shape = [jax.ShapeDtypeStruct((1, 1, 3, kind.count), F32)]
    if not has_layers:
        out_shape.append(jax.ShapeDtypeStruct((STEPS, width, 4, LANES), F32))
    vmem = pl.BlockSpec(memory_space=pltpu.VMEM)
    hbm = pl.BlockSpec(memory_space=pl.ANY)
    n_layers = len(layers) if has_layers else 0
    return pl.pallas_call(
        functools.partial(sim_kernel, kind, width, unroll, groups, offsets, has_layers),
        out_shape=out_shape,
        in_specs=[hbm] * len(bufs) + [vmem] * (2 + n_layers),
        out_specs=[vmem] * len(out_shape),
        scratch_shapes=[
            pltpu.VMEM((width, kind.rows, LANES), F32),
            pltpu.SemaphoreType.DMA((len(bufs),)),
        ]
        + scratch_of(kind, width, unroll),
        cost_estimate=pl.CostEstimate(flops=10**9, bytes_accessed=10**6, transcendentals=0),
        name="site_sim" if has_layers else "reg_sim",
    )(*bufs, *tables, *(layers or ()))


def pack_kernel(reg, site, site_from, *refs):
    (reg_disp, reg_vel, site_disp, site_vel, reg_nodes, site_nodes, reg_coefs, site_coefs,
     reg_minv, site_minv, reg_send, reg_recv, site_send, site_recv, slot_fill,
     layer_src, layer_fill, layer_dst, layer_stiff, reg_out, site_out) = refs
    grp = lax.axis_index("grp")

    @pl.when(grp < site_from)
    def _():
        fill = [slot_fill[0, 0, k] for k in range(2)]
        pack_kind(reg, reg_out, reg_disp, reg_vel, reg_nodes, reg_coefs, reg_minv,
                  reg_send, reg_recv, fill, (layer_src, layer_fill[0, 0]))

    @pl.when(grp >= site_from)
    def _():
        fill = [slot_fill[0, 0, k] for k in range(2, 4)]
        pack_kind(site, site_out, site_disp, site_vel, site_nodes, site_coefs, site_minv,
                  site_send, site_recv, fill, (layer_dst, layer_stiff))


def tables_of(kind, table):
    size = kind.quads_pad
    parts = [
        jnp.pad(
            table[a * kind.quads : (a + 1) * kind.quads],
            ((0, size - kind.quads), (0, kind.points_pad - kind.points)),
        )
        for a in range(3)
    ]
    whole = jnp.concatenate(parts, axis=0)
    high = lax.reduce_precision(whole, 8, 7)
    low = lax.reduce_precision(whole - high, 8, 7)
    first = jnp.concatenate([high, low, high], axis=1)
    first = jnp.pad(first, ((0, 0), (0, kind.depth_in - first.shape[1])))
    second = -jnp.concatenate([high.T, low.T, high.T], axis=1)
    second = jnp.pad(second, ((0, 0), (0, kind.depth_out - second.shape[1])))
    return first.astype(BF16), second.astype(BF16)


def gather_window(value, groups, offsets, count):
    chips = count // 2
    low, high = groups

    def moved(array, chip_shift, flip):
        route = []
        for grp in range(low, high):
            for index in range(count):
                chip, core = divmod(index, 2)
                target = ((chip + chip_shift) % chips) * 2 + (core ^ flip)
                route.append((grp * count + index, grp * count + target))
        return lax.ppermute(array, ("grp", "sub"), route)

    by_chip = [value if shift % chips == 0 else moved(value, shift, 0) for shift in offsets]
    result = []
    for array in by_chip:
        result += [array, moved(array, 0, 1)]
    return result


def shards(
    reg_disp, reg_vel, site_disp, site_vel, reg_nodes, site_nodes, reg_coefs, site_coefs,
    reg_table, site_table, reg_minv, site_minv, reg_send, reg_recv, site_send, site_recv,
    slot_fill, layer_src, layer_fill, layer_dst, layer_stiff,
):
    group_count = lax.axis_size("grp")
    count = lax.axis_size("sub")
    site_groups = group_count // 4
    reg_groups = 3 * site_groups
    slots = reg_send.shape[-1]
    reg = Kind(reg_nodes, reg_coefs, reg_disp, slots, 0)
    site = Kind(site_nodes, site_coefs, site_disp, slots, 3)
    unroll = min(UNROLL, count)
    width = min(count, up_to(2 * STEPS + 1, unroll))
    chips = count // 2
    reach = STEPS // 2
    if 2 * reach + 1 >= chips:
        offsets = tuple(range(chips))
    else:
        offsets = tuple(range(-reach, reach + 1))

    vmem = pl.BlockSpec(memory_space=pltpu.VMEM)
    smem = pl.BlockSpec(memory_space=pltpu.SMEM)
    reg_buf, site_buf = pl.pallas_call(
        functools.partial(pack_kernel, reg, site, reg_groups),
        out_shape=[
            jax.ShapeDtypeStruct((reg.rows, LANES), F32),
            jax.ShapeDtypeStruct((site.rows, LANES), F32),
        ],
        in_specs=[vmem] * 14 + [smem, vmem, smem, vmem, vmem],
        out_specs=[vmem] * 2,
        name="pack",
    )(
        reg_disp, reg_vel, site_disp, site_vel, reg_nodes, site_nodes, reg_coefs, site_coefs,
        reg_minv, site_minv, reg_send, reg_recv, site_send, site_recv, slot_fill,
        layer_src, layer_fill, layer_dst, layer_stiff,
    )
    reg_tables = tables_of(reg, reg_table)
    site_tables = tables_of(site, site_table)
    reg_bufs = gather_window(reg_buf, (0, reg_groups), offsets, count)
    site_bufs = gather_window(site_buf, (reg_groups, group_count), offsets, count)
    reg_final, layer_out = run_sim(
        reg, width, unroll, (0, reg_groups), offsets, reg_bufs, reg_tables, None
    )
    layers = [
        lax.ppermute(
            layer_out,
            "grp",
            [(m * site_groups + i, reg_groups + i) for i in range(site_groups)],
        )
        for m in range(3)
    ]
    (site_final,) = run_sim(
        site, width, unroll, (reg_groups, group_count), offsets, site_bufs, site_tables, layers
    )
    return reg_final, site_final


def solution(mesh):
    def spec(rank):
        return P("grp", "sub", *([None] * (rank - 2)))

    ranks = (4, 4, 4, 4, 4, 4, 6, 6, 0, 0, 3, 3, 4, 4, 4, 4, 3, 3, 2, 4, 4)
    return jax.shard_map(
        shards,
        mesh=mesh,
        in_specs=tuple(spec(rank) if rank else P() for rank in ranks),
        out_specs=(spec(4), spec(4)),
        check_vma=False,
    )
```

```python
import functools

import jax
import jax.numpy as jnp
from jax import lax
from jax.experimental import pallas as pl
from jax.experimental.pallas import tpu as pltpu
from jax.sharding import PartitionSpec as P

STEPS = 8
UNROLL = 8
LANES = 128
F32 = jnp.float32
BF16 = jnp.bfloat16
PAIRS = ((0, 0), (0, 1), (0, 2), (1, 1), (1, 2), (2, 2))
PAIR_OF = {**{ab: i for i, ab in enumerate(PAIRS)}, **{ab[::-1]: i for i, ab in enumerate(PAIRS)}}


def up_to(value, unit):
    return -(-value // unit) * unit


class Kind:
    def __init__(self, nodes, coefs, disp, sources):
        self.points, self.elems = nodes.shape[-2:]
        self.quads = coefs.shape[-2]
        self.count = disp.shape[-1]
        self.blocks = self.count // LANES
        self.cuts = self.elems // LANES
        self.points_pad = up_to(self.points, 8)
        self.quads_pad = up_to(self.quads, 8)
        self.blocks_pad = up_to(self.blocks, 2)
        self.depth_in = up_to(3 * self.points_pad, 16)
        self.depth_out = up_to(9 * self.quads_pad, 16)
        self.chunks = self.points * self.cuts
        self.sources = sources
        self.tiles = up_to(self.chunks, 4) // 4
        self.extra = 2 + sources
        self.extra_tiles = up_to(self.extra, 4) // 4
        self.table_turned = self.quads_pad == self.quads
        row = 0
        for name, rows in (
            ("coefs", 6 * self.quads * self.cuts),
            ("nodes", self.points * self.cuts),
            ("disp", 3 * self.blocks),
            ("vel", 3 * self.blocks),
            ("minv", self.blocks),
            ("send", 2),
            ("recv", 2),
            ("layer", 2 * sources if sources else 1),
        ):
            setattr(self, "at_" + name, row)
            row += rows
        self.rows = up_to(row, 8)


def pack_kernel(kind, *refs):
    disp, vel, nodes, coefs, minv, send, recv, fill, layer_a, layer_b, table, out, first, second = refs[:14]
    work = refs[14]
    for pair, (a, b) in enumerate(PAIRS):
        for cut in range(kind.cuts):
            at = kind.at_coefs + (pair * kind.cuts + cut) * kind.quads
            out[at : at + kind.quads, :] = coefs[0, 0, a, b, :, cut * LANES : (cut + 1) * LANES]
    for cut in range(kind.cuts):
        for p in range(kind.points):
            at = kind.at_nodes + cut * kind.points + p
            out[at : at + 1, :] = nodes[0, p, :, cut * LANES : (cut + 1) * LANES].astype(F32)
    for block in range(kind.blocks):
        lanes = slice(block * LANES, (block + 1) * LANES)
        for c in range(3):
            for at, ref in ((kind.at_disp, disp), (kind.at_vel, vel)):
                out[at + 3 * block + c : at + 3 * block + c + 1, :] = ref[0, c, :, lanes]
        out[kind.at_minv + block : kind.at_minv + block + 1, :] = minv[0, 0:1, lanes]
    lane = lax.broadcasted_iota(jnp.int32, (1, LANES), 1)
    for side in range(2):
        live = lane < fill[0, 0, (2 if kind.sources else 0) + side]
        row = send[0, 0, side : side + 1, :]
        out[kind.at_send + side : kind.at_send + side + 1, :] = jnp.where(live, row, -1).astype(F32)
    out[kind.at_recv : kind.at_recv + 2, :] = recv[0, 0].astype(F32)
    for m in range(kind.sources):
        at = kind.at_layer + m
        out[at : at + 1, :] = layer_a[0, m].astype(F32)
        out[at + kind.sources : at + kind.sources + 1, :] = layer_b[0, m]
    if not kind.sources:
        row = layer_a[0, 0:1, :]
        live = lane < layer_b[0, 0]
        out[kind.at_layer : kind.at_layer + 1, :] = jnp.where(live, row, -1).astype(F32)
    size = kind.quads_pad
    work[...] = jnp.zeros(work.shape, F32)
    if kind.table_turned:
        work[0 : kind.points, 0 : 3 * kind.quads] = table[...]
        turned = work[...]
        plain = jnp.transpose(turned)
    else:
        for a in range(3):
            work[a * size : a * size + kind.quads, 0 : kind.points] = table[
                a * kind.quads : (a + 1) * kind.quads, :
            ]
        plain = work[...]
        turned = jnp.transpose(plain)
    step = kind.points_pad
    high = high_part(plain)
    low = plain - high
    rows = high + pltpu.roll(low, step, 1) + pltpu.roll(high, 2 * step, 1)
    first[...] = rows[0 : 3 * size, 0 : kind.depth_in].astype(BF16)
    high = high_part(turned)
    low = turned - high
    wide = jnp.zeros((LANES, LANES), F32)
    high = jnp.concatenate([high, wide], axis=1)
    low = jnp.concatenate([low, wide], axis=1)
    rows = high + pltpu.roll(low, 3 * size, 1) + pltpu.roll(high, 6 * size, 1)
    second[...] = (-rows[0 : kind.points_pad, 0 : kind.depth_out]).astype(BF16)


def pack(kind, disp, vel, nodes, coefs, minv, send, recv, fill, layer_a, layer_b, table):
    def thin(array):
        return jnp.transpose(array, (0, 2, 1, 3))

    vmem = pl.BlockSpec(memory_space=pltpu.VMEM)
    smem = pl.BlockSpec(memory_space=pltpu.SMEM)
    if kind.sources:
        layer_a, layer_b = thin(layer_a), thin(layer_b)
    if kind.table_turned:
        table = table.T
    return pl.pallas_call(
        functools.partial(pack_kernel, kind),
        out_shape=[
            jax.ShapeDtypeStruct((kind.rows, LANES), F32),
            jax.ShapeDtypeStruct((3 * kind.quads_pad, kind.depth_in), BF16),
            jax.ShapeDtypeStruct((kind.points_pad, kind.depth_out), BF16),
        ],
        in_specs=[vmem] * 7 + [smem, vmem, vmem if kind.sources else smem, vmem],
        out_specs=[vmem] * 3,
        scratch_shapes=[pltpu.VMEM((LANES, LANES), F32)],
        name="site_pack" if kind.sources else "reg_pack",
    )(thin(disp), thin(vel), thin(nodes), coefs, minv, send, recv, fill, layer_a, layer_b, table)


def split_index(value):
    index = value.astype(jnp.int32)
    return index & (LANES - 1), index >> 7


def high_part(value):
    return value.astype(BF16).astype(F32)


def simulate(kind, width, unroll, buf, lhs_in, lhs_out, layers, emit, s):
    points, cuts, blocks = kind.points, kind.cuts, kind.blocks
    quads_pad = kind.quads_pad
    half_rows = 8 * kind.blocks_pad
    row8 = lax.broadcasted_iota(jnp.int32, (8, LANES), 0)
    low_half = row8 < 4
    row16 = lax.broadcasted_iota(jnp.int32, (16, LANES), 0)
    block_ids = [
        jnp.where(row16 < 8, 2 * j, 2 * j + 1).astype(F32).astype(BF16)
        for j in range(kind.blocks_pad // 2)
    ]
    zero16 = jnp.zeros((16, LANES), BF16)
    zero8 = jnp.zeros((8, LANES), F32)
    lane_ids = lax.broadcasted_iota(jnp.int32, (LANES, LANES), 1).astype(F32).astype(BF16)
    one = jnp.ones((LANES, LANES), BF16)
    none = jnp.zeros((LANES, LANES), BF16)
    main_rows = kind.tiles * 256

    def onehot(q, chunk_no, base_row, columns, at):
        hit = columns[:, at : at + 1] == lane_ids
        tile, half, part = chunk_no // 4, (chunk_no // 2) % 2, chunk_no % 2
        rows = pl.ds(base_row + tile * 256 + part * LANES, LANES)
        s.onehot[q, half, rows, :] = jnp.where(hit, one, none)

    def hold_block(q, chunk_no, hi_row):
        s.block_of[q, chunk_no : chunk_no + 1, :] = hi_row.astype(F32)

    def columns_of(rows):
        count = rows.shape[0]
        if count < LANES:
            rows = jnp.concatenate([rows, jnp.zeros((LANES - count, LANES), F32)], axis=0)
        return jnp.transpose(rows).astype(BF16)

    def setup(q, _):
        for pair in range(6):
            for cut in range(cuts):
                at = kind.at_coefs + (pair * cuts + cut) * kind.quads
                lanes = slice(cut * LANES, (cut + 1) * LANES)
                if kind.quads_pad > kind.quads:
                    s.coefs[q, pair, :, lanes] = jnp.zeros((quads_pad, LANES), F32)
                s.coefs[q, pair, 0 : kind.quads, lanes] = buf[q, at : at + kind.quads, :]
        for cut in range(cuts):
            at = kind.at_nodes + cut * points
            value = buf[q, at : at + points, :]
            lo, hi = split_index(value)
            if kind.points_pad > points:
                s.lo[q, cut] = jnp.zeros((kind.points_pad, LANES), jnp.int32)
                s.hi[q, cut] = jnp.zeros((kind.points_pad, LANES), jnp.int32)
            s.lo[q, cut, 0:points, :] = lo
            s.hi[q, cut, 0:points, :] = hi
            columns = columns_of(lo.astype(F32))
            for p in range(points):
                onehot(q, cut * points + p, 0, columns, p)
                hold_block(q, cut * points + p, hi[p : p + 1, :])
        for chunk in range(kind.chunks, 4 * kind.tiles):
            columns = jnp.zeros((LANES, LANES), BF16)
            onehot(q, chunk, 0, columns, 0)
            hold_block(q, chunk, jnp.zeros((1, LANES), jnp.int32))
        extra = [buf[q, kind.at_recv : kind.at_recv + 2, :]]
        if kind.sources:
            extra.append(buf[q, kind.at_layer : kind.at_layer + kind.sources, :])
        extra.append(jnp.zeros((4 * kind.extra_tiles - kind.extra, LANES), F32))
        lo, hi = split_index(jnp.concatenate([e for e in extra if e.shape[0]], axis=0))
        columns = columns_of(lo.astype(F32))
        for chunk in range(4 * kind.extra_tiles):
            onehot(q, chunk, main_rows, columns, chunk)
            hold_block(q, 4 * kind.tiles + chunk, hi[chunk : chunk + 1, :])
        send_rows = [
            jnp.broadcast_to(buf[q, kind.at_send + side : kind.at_send + side + 1, :], (4, LANES))
            for side in range(2)
        ]
        s.send_lo[q], s.send_hi[q] = split_index(jnp.concatenate(send_rows, axis=0))
        if not kind.sources:
            row = buf[q, kind.at_layer : kind.at_layer + 1, :]
            s.layer_lo[q], s.layer_hi[q] = split_index(jnp.broadcast_to(row, (8, LANES)))
        for block in range(blocks):
            at = kind.at_disp + 3 * block
            now = buf[q, at : at + 3, :]
            at = kind.at_vel + 3 * block
            before = now - buf[q, at : at + 3, :]
            for ref, value in ((s.now, now), (s.before, before)):
                ref[q, block] = zero8
                ref[q, block, 0:3, :] = value
                ref[q, block, 4:7, :] = value
        return 0

    lax.fori_loop(0, width, setup, 0)
    for lane in range(unroll):
        s.parts[lane] = jnp.zeros(s.parts.shape[1:], F32)
    s.sends[0] = zero8
    s.sends[width + 1] = zero8

    def spread(q, first, values):
        blank = jnp.zeros((half_rows, LANES), BF16)
        parts = []
        for number, value8 in enumerate(values):
            doubled = jnp.concatenate([value8, value8], axis=0).astype(BF16)
            held = s.block_of[q, first + number : first + number + 1, :]
            held = jnp.broadcast_to(held, (16, LANES)).astype(BF16)
            parts.append(
                jnp.concatenate(
                    [jnp.where(held == ids, doubled, zero16) for ids in block_ids], axis=0
                )
            )
        parts += [blank] * (4 - len(values))
        return jnp.concatenate(
            [jnp.concatenate(parts[0:2], axis=1), jnp.concatenate(parts[2:4], axis=1)], axis=0
        )

    def scattered(q, first, rows_from, get, count):
        total = None
        for at in range(0, count, 4):
            left = spread(q, first + at, [get(k) for k in range(at, min(at + 4, count))])
            rows = slice(rows_from + at * 64, rows_from + at * 64 + 256)
            right = jnp.concatenate([s.onehot[q, half, rows, :] for half in range(2)], axis=1)
            term = jnp.dot(left, right, preferred_element_type=F32)
            total = term if total is None else total + term
        return total

    def fold(total, block):
        rows = slice(block * 8, block * 8 + 8)
        other = slice(half_rows + block * 8, half_rows + block * 8 + 8)
        value = total[rows, 0:LANES] + total[other, LANES : 2 * LANES]
        return value + pltpu.roll(value, 4, 0)

    def choose(found, bits):
        for bit in bits:
            found = [
                jnp.where(bit, found[k + 1], found[k]) if k + 1 < len(found) else found[k]
                for k in range(0, len(found), 2)
            ]
        return found[0]

    def bits_of(hi):
        count = (blocks - 1).bit_length()
        return [(hi & (1 << k)) != 0 for k in range(count)]

    def lookup(row, lo):
        return jnp.take_along_axis(row, lo, axis=1, mode="promise_in_bounds")

    def pick(source, lo, hi):
        found = [lookup(source(block), lo) for block in range(blocks)]
        return jnp.where(hi < 0, 0.0, choose(found, bits_of(hi)))

    def force(q, lane):
        stacked = []
        picked = {}
        for cut in range(cuts):
            groups = {c: [] for c in range(3)}
            for at in range(0, kind.points_pad, 8):
                lo = s.lo[q, cut, at : at + 8, :]
                bits = bits_of(s.hi[q, cut, at : at + 8, :])
                for c in range(3):
                    found = [
                        lookup(jnp.broadcast_to(s.now[q, block, c : c + 1, :], (8, LANES)), lo)
                        for block in range(blocks)
                    ]
                    groups[c].append(choose(found, bits))
            for c in range(3):
                picked[c, cut] = jnp.concatenate(groups[c], axis=0)
        order = [(c, cut) for c in range(3) for cut in range(cuts)]
        for key in order:
            high = high_part(picked[key])
            rows = [high, high, picked[key] - high]
            pad = kind.depth_in - 3 * kind.points_pad
            if pad:
                rows.append(jnp.zeros((pad, LANES), F32))
            stacked.append(jnp.concatenate(rows, axis=0).astype(BF16))
        grad = jnp.dot(
            lhs_in[...], jnp.concatenate(stacked, axis=1), preferred_element_type=F32
        )
        stacked = []
        for number, (c, cut) in enumerate(order):
            lanes = slice(number * LANES, (number + 1) * LANES)
            cut_lanes = slice(cut * LANES, (cut + 1) * LANES)
            pieces = [grad[b * quads_pad : (b + 1) * quads_pad, lanes] for b in range(3)]
            coef = [s.coefs[q, pair, :, cut_lanes] for pair in range(6)]
            flux = jnp.concatenate(
                [
                    coef[PAIR_OF[a, 0]] * pieces[0]
                    + coef[PAIR_OF[a, 1]] * pieces[1]
                    + coef[PAIR_OF[a, 2]] * pieces[2]
                    for a in range(3)
                ],
                axis=0,
            )
            high = high_part(flux)
            rows = [high, high, flux - high]
            pad = kind.depth_out - 9 * quads_pad
            if pad:
                rows.append(jnp.zeros((pad, LANES), F32))
            stacked.append(jnp.concatenate(rows, axis=0).astype(BF16))
        elem = jnp.dot(
            lhs_out[...], jnp.concatenate(stacked, axis=1), preferred_element_type=F32
        )
        for number, (c, cut) in enumerate(order):
            value = elem[:, number * LANES : (number + 1) * LANES]
            high = high_part(value)
            size = kind.points_pad
            s.parts[lane, cut, c * size : (c + 1) * size, :] = high
            s.parts[lane, cut, (c + 4) * size : (c + 5) * size, :] = value - high
        def entry(chunk):
            cut, p = divmod(chunk, points)
            return s.parts[lane, cut, pl.ds(p, 8, stride=kind.points_pad), :]

        total = scattered(q, 0, 0, entry, kind.chunks)
        folded = [fold(total, block) for block in range(blocks)]
        for block in range(blocks):
            s.force[q, block] = folded[block]
        s.sends[q + 1] = pick(lambda block: folded[block], s.send_lo[q], s.send_hi[q])

    def split8(value):
        high = high_part(value)
        return jnp.where(low_half, high, value - high)

    def update(q, lane, step):
        lower = s.sends[q]
        upper = s.sends[q + 2]
        values = [
            jnp.where(low_half, pltpu.roll(lower, 4, 0), lower),
            jnp.where(low_half, upper, pltpu.roll(upper, 4, 0)),
        ]
        for m in range(kind.sources):
            four = layers[m][step, q]
            at = kind.at_layer + kind.sources + m
            values.append(jnp.concatenate([four, four], axis=0) * buf[q, at : at + 1, :])
        total = scattered(
            q, 4 * kind.tiles, main_rows, lambda k: split8(values[k]), len(values)
        )
        after = []
        for block in range(blocks):
            now = s.now[q, block]
            scale = buf[q, kind.at_minv + block : kind.at_minv + block + 1, :]
            whole = s.force[q, block] + fold(total, block)
            value = 2.0 * now - s.before[q, block] + scale * whole
            s.before[q, block] = now
            s.now[q, block] = value
            after.append(value)
        if emit is not None:
            picked = pick(lambda block: after[block], s.layer_lo[q], s.layer_hi[q])
            emit[step, q] = picked[0:4]

    def one_step(step, _):
        def forces(group, _):
            for lane in range(unroll):
                force(group * unroll + lane, lane)
            return 0

        def updates(group, _):
            for lane in range(unroll):
                update(group * unroll + lane, lane, step)
            return 0

        lax.fori_loop(0, width // unroll, forces, 0)
        lax.fori_loop(0, width // unroll, updates, 0)
        return 0

    lax.fori_loop(0, STEPS, one_step, 0)


SCRATCH = (
    "onehot", "block_of", "coefs", "lo", "hi", "send_lo", "send_hi", "layer_lo", "layer_hi",
    "now", "before", "force", "sends", "parts",
)


def scratch_of(kind, width, unroll):
    tiles = kind.tiles + kind.extra_tiles
    return [
        pltpu.VMEM((width, 2, tiles * 256, LANES), BF16),
        pltpu.VMEM((width, 4 * tiles, LANES), F32),
        pltpu.VMEM((width, 6, kind.quads_pad, kind.elems), F32),
        pltpu.VMEM((width, kind.cuts, kind.points_pad, LANES), jnp.int32),
        pltpu.VMEM((width, kind.cuts, kind.points_pad, LANES), jnp.int32),
        pltpu.VMEM((width, 8, LANES), jnp.int32),
        pltpu.VMEM((width, 8, LANES), jnp.int32),
        pltpu.VMEM((width, 8, LANES), jnp.int32),
        pltpu.VMEM((width, 8, LANES), jnp.int32),
        pltpu.VMEM((width, kind.blocks, 8, LANES), F32),
        pltpu.VMEM((width, kind.blocks, 8, LANES), F32),
        pltpu.VMEM((width, kind.blocks, 8, LANES), F32),
        pltpu.VMEM((width + 2, 8, LANES), F32),
        pltpu.VMEM((unroll, kind.cuts, 8 * kind.points_pad, LANES), F32),
    ]


class Refs:
    pass


def window_base(index, count, width):
    return jnp.clip(index - STEPS, 0, count - width)


def sim_kernel(kind, width, unroll, offsets, spare, *refs):
    sub = lax.axis_index("sub")
    count = lax.axis_size("sub")
    chips = count // 2
    n_bufs = 2 * len(offsets)
    bufs, refs = refs[:n_bufs], refs[n_bufs:]
    lhs_in, lhs_out, refs = refs[0], refs[1], refs[2:]
    layers, refs = refs[: kind.sources], refs[kind.sources :]
    final, refs = refs[0], refs[1:]
    emit = None
    if not kind.sources:
        emit, refs = refs[0], refs[1:]
    refs = refs[spare:]
    buf, sem, refs = refs[0], refs[1], refs[2:]
    s = Refs()
    for name, ref in zip(SCRATCH, refs, strict=True):
        setattr(s, name, ref)
    base = window_base(sub, count, width)
    if width < count:
        buf[...] = jnp.zeros(buf.shape, F32)
    copies = []
    for number, offset in enumerate(offsets):
        for other in range(2):
            chip = lax.rem(sub // 2 - offset + chips, chips)
            core = lax.rem(sub, 2)
            slot = chip * 2 + (core if other == 0 else 1 - core) - base
            at = 2 * number + other
            inside = jnp.logical_and(slot >= 0, slot < width)
            slot = jnp.clip(slot, 0, width - 1)
            copy = pltpu.make_async_copy(bufs[at], buf.at[slot], sem.at[at])
            copies.append((inside, copy))
    for phase in ("start", "wait"):
        for inside, copy in copies:
            if width < count:
                pl.when(inside)(getattr(copy, phase))
            else:
                getattr(copy, phase)()
    simulate(kind, width, unroll, buf, lhs_in, lhs_out, layers, emit, s)
    for block in range(kind.blocks):
        for c in range(3):
            final[0, c, :, block * LANES : (block + 1) * LANES] = s.now[
                sub - base, block, c : c + 1, :
            ]


def run_sim(kind, width, unroll, offsets, bufs, tables, layers, spare):
    out_shape = [jax.ShapeDtypeStruct((1, 3, 1, kind.count), F32)]
    if not kind.sources:
        out_shape.append(jax.ShapeDtypeStruct((STEPS, width, 4, LANES), F32))
    vmem = pl.BlockSpec(memory_space=pltpu.VMEM)
    hbm = pl.BlockSpec(memory_space=pl.ANY)
    return pl.pallas_call(
        functools.partial(sim_kernel, kind, width, unroll, offsets, len(spare)),
        out_shape=out_shape + spare,
        in_specs=[hbm] * len(bufs) + [vmem] * (2 + len(layers)),
        out_specs=[vmem] * len(out_shape) + [hbm] * len(spare),
        scratch_shapes=[
            pltpu.VMEM((width, kind.rows, LANES), F32),
            pltpu.SemaphoreType.DMA((len(bufs),)),
        ]
        + scratch_of(kind, width, unroll),
        name="site_sim" if kind.sources else "reg_sim",
    )(*bufs, *tables, *layers)


def blank_kernel(final, *rest):
    final[...] = jnp.zeros(final.shape, F32)


def gather_window(value, groups, offsets, count):
    chips = count // 2
    low, high = groups

    def moved(array, chip_shift, flip):
        route = []
        for grp in range(low, high):
            for index in range(count):
                chip, core = divmod(index, 2)
                target = ((chip + chip_shift) % chips) * 2 + (core ^ flip)
                route.append((grp * count + index, grp * count + target))
        return lax.ppermute(array, ("grp", "sub"), route)

    by_chip = [value if shift % chips == 0 else moved(value, shift, 0) for shift in offsets]
    result = []
    for array in by_chip:
        result += [array, moved(array, 0, 1)]
    return result


def shards(
    reg_disp, reg_vel, site_disp, site_vel, reg_nodes, site_nodes, reg_coefs, site_coefs,
    reg_table, site_table, reg_minv, site_minv, reg_send, reg_recv, site_send, site_recv,
    slot_fill, layer_src, layer_fill, layer_dst, layer_stiff,
):
    group_count = lax.axis_size("grp")
    count = lax.axis_size("sub")
    site_groups = group_count // 4
    reg_groups = 3 * site_groups
    reg = Kind(reg_nodes, reg_coefs, reg_disp, 0)
    site = Kind(site_nodes, site_coefs, site_disp, 3)
    unroll = min(UNROLL, count)
    width = min(count, up_to(2 * STEPS + 1, unroll))
    chips = count // 2
    reach = STEPS // 2
    if 2 * reach + 1 >= chips:
        offsets = tuple(range(chips))
    else:
        offsets = tuple(range(-reach, reach + 1))
    is_site = lax.axis_index("grp") >= reg_groups
    vmem = pl.BlockSpec(memory_space=pltpu.VMEM)
    hbm = pl.BlockSpec(memory_space=pl.ANY)
    site_spare = [jax.ShapeDtypeStruct((site.rows, LANES), F32)] * (2 * len(offsets)) + [
        jax.ShapeDtypeStruct((3 * site.quads_pad, site.depth_in), BF16),
        jax.ShapeDtypeStruct((site.points_pad, site.depth_out), BF16),
    ]

    def regional():
        buf, *tables = pack(
            reg, reg_disp, reg_vel, reg_nodes, reg_coefs, reg_minv, reg_send, reg_recv,
            slot_fill, layer_src, layer_fill, reg_table,
        )
        bufs = gather_window(buf, (0, reg_groups), offsets, count)
        final, layer, *spare = run_sim(reg, width, unroll, offsets, bufs, tables, (), site_spare)
        return (final, layer, *spare)

    def prepare_site():
        buf, *tables = pack(
            site, site_disp, site_vel, site_nodes, site_coefs, site_minv, site_send, site_recv,
            slot_fill, layer_dst, layer_stiff, site_table,
        )
        bufs = gather_window(buf, (reg_groups, group_count), offsets, count)
        final, layer = pl.pallas_call(
            blank_kernel,
            out_shape=[
                jax.ShapeDtypeStruct((1, 3, 1, reg.count), F32),
                jax.ShapeDtypeStruct((STEPS, width, 4, LANES), F32),
            ],
            out_specs=[vmem, hbm],
            name="blank",
        )()
        return (final, layer, *bufs, *tables)

    reg_final, layer_out, *rest = lax.cond(is_site, prepare_site, regional)
    site_bufs, site_tables = rest[:-2], rest[-2:]
    layers = [
        lax.ppermute(
            layer_out,
            "grp",
            [(m * site_groups + i, reg_groups + i) for i in range(site_groups)],
        )
        for m in range(3)
    ]

    def run_site():
        return run_sim(site, width, unroll, offsets, site_bufs, site_tables, layers, [])[0]

    def no_site():
        return jnp.zeros((1, 3, 1, site.count), F32)

    site_final = lax.cond(is_site, run_site, no_site)
    return jnp.transpose(reg_final, (0, 2, 1, 3)), jnp.transpose(site_final, (0, 2, 1, 3))


def solution(mesh):
    def spec(rank):
        return P("grp", "sub", *([None] * (rank - 2)))

    ranks = (4, 4, 4, 4, 4, 4, 6, 6, 0, 0, 3, 3, 4, 4, 4, 4, 3, 3, 2, 4, 4)
    return jax.shard_map(
        shards,
        mesh=mesh,
        in_specs=tuple(spec(rank) if rank else P() for rank in ranks),
        out_specs=(spec(4), spec(4)),
        check_vma=False,
    )
```

```python
import functools

import jax
import jax.numpy as jnp
from jax import lax
from jax.experimental import pallas as pl
from jax.experimental.pallas import tpu as pltpu
from jax.sharding import PartitionSpec as P

STEPS = 8
UNROLL = 8
LANES = 128
F32 = jnp.float32
BF16 = jnp.bfloat16
PAIRS = ((0, 0), (0, 1), (0, 2), (1, 1), (1, 2), (2, 2))
PAIR_OF = {**{ab: i for i, ab in enumerate(PAIRS)}, **{ab[::-1]: i for i, ab in enumerate(PAIRS)}}


def up_to(value, unit):
    return -(-value // unit) * unit


class Kind:
    def __init__(self, nodes, coefs, disp, sources):
        self.points, self.elems = nodes.shape[-2:]
        self.quads = coefs.shape[-2]
        self.count = disp.shape[-1]
        self.blocks = self.count // LANES
        self.cuts = self.elems // LANES
        self.points_pad = up_to(self.points, 8)
        self.quads_pad = up_to(self.quads, 8)
        self.blocks_pad = up_to(self.blocks, 2)
        self.depth_in = up_to(3 * self.points_pad, 16)
        self.depth_out = up_to(9 * self.quads_pad, 16)
        self.chunks = self.points * self.cuts
        self.sources = sources
        self.dense = self.blocks >= 8 and self.blocks % 4 == 0
        self.tiles = up_to(self.chunks, 4) // 4
        self.extra = 2 + sources
        self.extra_tiles = up_to(self.extra, 4) // 4
        self.table_turned = self.quads_pad == self.quads
        row = 0
        for name, rows in (
            ("coefs", 6 * self.quads * self.cuts),
            ("nodes", self.points * self.cuts),
            ("disp", 3 * self.blocks),
            ("vel", 3 * self.blocks),
            ("minv", self.blocks),
            ("send", 2),
            ("recv", 2),
            ("layer", 2 * sources if sources else 1),
        ):
            setattr(self, "at_" + name, row)
            row += rows
        self.rows = up_to(row, 8)


def pack_kernel(kind, *refs):
    disp, vel, nodes, coefs, minv, send, recv, fill, layer_a, layer_b, table, out, first, second = refs[:14]
    work = refs[14]
    for pair, (a, b) in enumerate(PAIRS):
        for cut in range(kind.cuts):
            at = kind.at_coefs + (pair * kind.cuts + cut) * kind.quads
            out[at : at + kind.quads, :] = coefs[0, 0, a, b, :, cut * LANES : (cut + 1) * LANES]
    for cut in range(kind.cuts):
        for p in range(kind.points):
            at = kind.at_nodes + cut * kind.points + p
            out[at : at + 1, :] = nodes[0, p, :, cut * LANES : (cut + 1) * LANES].astype(F32)
    for block in range(kind.blocks):
        lanes = slice(block * LANES, (block + 1) * LANES)
        for c in range(3):
            for at, ref in ((kind.at_disp, disp), (kind.at_vel, vel)):
                out[at + 3 * block + c : at + 3 * block + c + 1, :] = ref[0, c, :, lanes]
        out[kind.at_minv + block : kind.at_minv + block + 1, :] = minv[0, 0:1, lanes]
    lane = lax.broadcasted_iota(jnp.int32, (1, LANES), 1)
    for side in range(2):
        live = lane < fill[0, 0, (2 if kind.sources else 0) + side]
        row = send[0, 0, side : side + 1, :]
        out[kind.at_send + side : kind.at_send + side + 1, :] = jnp.where(live, row, -1).astype(F32)
    out[kind.at_recv : kind.at_recv + 2, :] = recv[0, 0].astype(F32)
    for m in range(kind.sources):
        at = kind.at_layer + m
        out[at : at + 1, :] = layer_a[0, m].astype(F32)
        out[at + kind.sources : at + kind.sources + 1, :] = layer_b[0, m]
    if not kind.sources:
        row = layer_a[0, 0:1, :]
        live = lane < layer_b[0, 0]
        out[kind.at_layer : kind.at_layer + 1, :] = jnp.where(live, row, -1).astype(F32)
    size = kind.quads_pad
    work[...] = jnp.zeros(work.shape, F32)
    if kind.table_turned:
        work[0 : kind.points, 0 : 3 * kind.quads] = table[...]
        turned = work[...]
        plain = jnp.transpose(turned)
    else:
        for a in range(3):
            work[a * size : a * size + kind.quads, 0 : kind.points] = table[
                a * kind.quads : (a + 1) * kind.quads, :
            ]
        plain = work[...]
        turned = jnp.transpose(plain)
    step = kind.points_pad
    high = high_part(plain)
    low = plain - high
    rows = high + pltpu.roll(low, step, 1) + pltpu.roll(high, 2 * step, 1)
    first[...] = rows[0 : 3 * size, 0 : kind.depth_in].astype(BF16)
    high = high_part(turned)
    low = turned - high
    wide = jnp.zeros((LANES, LANES), F32)
    high = jnp.concatenate([high, wide], axis=1)
    low = jnp.concatenate([low, wide], axis=1)
    rows = high + pltpu.roll(low, 3 * size, 1) + pltpu.roll(high, 6 * size, 1)
    second[...] = (-rows[0 : kind.points_pad, 0 : kind.depth_out]).astype(BF16)


def pack(kind, disp, vel, nodes, coefs, minv, send, recv, fill, layer_a, layer_b, table):
    def thin(array):
        return jnp.transpose(array, (0, 2, 1, 3))

    vmem = pl.BlockSpec(memory_space=pltpu.VMEM)
    smem = pl.BlockSpec(memory_space=pltpu.SMEM)
    if kind.sources:
        layer_a, layer_b = thin(layer_a), thin(layer_b)
    if kind.table_turned:
        table = table.T
    return pl.pallas_call(
        functools.partial(pack_kernel, kind),
        out_shape=[
            jax.ShapeDtypeStruct((kind.rows, LANES), F32),
            jax.ShapeDtypeStruct((3 * kind.quads_pad, kind.depth_in), BF16),
            jax.ShapeDtypeStruct((kind.points_pad, kind.depth_out), BF16),
        ],
        in_specs=[vmem] * 7 + [smem, vmem, vmem if kind.sources else smem, vmem],
        out_specs=[vmem] * 3,
        scratch_shapes=[pltpu.VMEM((LANES, LANES), F32)],
        name="site_pack" if kind.sources else "reg_pack",
    )(thin(disp), thin(vel), thin(nodes), coefs, minv, send, recv, fill, layer_a, layer_b, table)


def split_index(value):
    index = value.astype(jnp.int32)
    return index & (LANES - 1), index >> 7


def high_part(value):
    return value.astype(BF16).astype(F32)


def simulate(kind, width, unroll, own, mode, buf, lhs_in, lhs_out, layers, emit, begun, s):
    points, cuts, blocks = kind.points, kind.cuts, kind.blocks
    quads_pad = kind.quads_pad
    half_rows = 6 * blocks if kind.dense else 8 * kind.blocks_pad
    row8 = lax.broadcasted_iota(jnp.int32, (8, LANES), 0)
    low_half = row8 < 4
    row16 = lax.broadcasted_iota(jnp.int32, (16, LANES), 0)
    block_ids = [
        jnp.where(row16 < 8, 2 * j, 2 * j + 1).astype(F32).astype(BF16)
        for j in range(kind.blocks_pad // 2)
    ]
    zero16 = jnp.zeros((16, LANES), BF16)
    zero8 = jnp.zeros((8, LANES), F32)
    lane_ids = lax.broadcasted_iota(jnp.int32, (LANES, LANES), 1).astype(F32).astype(BF16)
    one = jnp.ones((LANES, LANES), BF16)
    none = jnp.zeros((LANES, LANES), BF16)
    main_rows = kind.tiles * 256

    def onehot(q, chunk_no, base_row, columns, at):
        hit = columns[:, at : at + 1] == lane_ids
        tile, half, part = chunk_no // 4, (chunk_no // 2) % 2, chunk_no % 2
        rows = pl.ds(base_row + tile * 256 + part * LANES, LANES)
        s.onehot[q, half, rows, :] = jnp.where(hit, one, none)

    def hold_block(q, chunk_no, hi_row):
        s.block_of[q, chunk_no : chunk_no + 1, :] = hi_row.astype(F32)

    def columns_of(rows):
        count = rows.shape[0]
        if count < LANES:
            rows = jnp.concatenate([rows, jnp.zeros((LANES - count, LANES), F32)], axis=0)
        return jnp.transpose(rows).astype(BF16)

    def setup(q, _):
        for pair in range(6):
            for cut in range(cuts):
                at = kind.at_coefs + (pair * cuts + cut) * kind.quads
                lanes = slice(cut * LANES, (cut + 1) * LANES)
                if kind.quads_pad > kind.quads:
                    s.coefs[q, pair, :, lanes] = jnp.zeros((quads_pad, LANES), F32)
                s.coefs[q, pair, 0 : kind.quads, lanes] = buf[q, at : at + kind.quads, :]
        for cut in range(cuts):
            at = kind.at_nodes + cut * points
            value = buf[q, at : at + points, :]
            lo, hi = split_index(value)
            if kind.points_pad > points:
                s.lo[q, cut] = jnp.zeros((kind.points_pad, LANES), jnp.int32)
                s.hi[q, cut] = jnp.zeros((kind.points_pad, LANES), jnp.int32)
            s.lo[q, cut, 0:points, :] = lo
            s.hi[q, cut, 0:points, :] = hi
            columns = columns_of(lo.astype(F32))
            for p in range(points):
                onehot(q, cut * points + p, 0, columns, p)
                hold_block(q, cut * points + p, hi[p : p + 1, :])
        for chunk in range(kind.chunks, 4 * kind.tiles):
            columns = jnp.zeros((LANES, LANES), BF16)
            onehot(q, chunk, 0, columns, 0)
            hold_block(q, chunk, jnp.zeros((1, LANES), jnp.int32))
        extra = [buf[q, kind.at_recv : kind.at_recv + 2, :]]
        if kind.sources:
            extra.append(buf[q, kind.at_layer : kind.at_layer + kind.sources, :])
        extra.append(jnp.zeros((4 * kind.extra_tiles - kind.extra, LANES), F32))
        lo, hi = split_index(jnp.concatenate([e for e in extra if e.shape[0]], axis=0))
        columns = columns_of(lo.astype(F32))
        for chunk in range(4 * kind.extra_tiles):
            onehot(q, chunk, main_rows, columns, chunk)
            hold_block(q, 4 * kind.tiles + chunk, hi[chunk : chunk + 1, :])
        send_rows = [
            jnp.broadcast_to(buf[q, kind.at_send + side : kind.at_send + side + 1, :], (4, LANES))
            for side in range(2)
        ]
        s.send_lo[q], s.send_hi[q] = split_index(jnp.concatenate(send_rows, axis=0))
        if not kind.sources:
            row = buf[q, kind.at_layer : kind.at_layer + 1, :]
            s.layer_lo[q], s.layer_hi[q] = split_index(jnp.broadcast_to(row, (8, LANES)))
        for block in range(blocks):
            at = kind.at_disp + 3 * block
            now = buf[q, at : at + 3, :]
            at = kind.at_vel + 3 * block
            before = now - buf[q, at : at + 3, :]
            for ref, value in ((s.now, now), (s.before, before)):
                ref[q, block] = zero8
                ref[q, block, 0:3, :] = value
                ref[q, block, 4:7, :] = value
        return 0

    def setup_pair(pair, _):
        for k in range(2):
            setup(2 * pair + k, 0)
        return 0

    lax.fori_loop(0, width // 2, setup_pair, 0)
    for lane in range(unroll):
        s.parts[lane] = jnp.zeros(s.parts.shape[1:], F32)
        s.turn[lane] = jnp.zeros(s.turn.shape[1:], F32)
    s.sends[0] = zero8
    s.sends[width + 1] = zero8

    slabs = half_rows // 8
    slab_rows = [
        [divmod(8 * slab + row, blocks) for row in range(8)] for slab in range(slabs)
    ]
    slab_ids = {}
    for slab in range(slabs if kind.dense else 0):
        number = slab_rows[slab][0][1]
        if number not in slab_ids:
            slab_ids[number] = lax.rem(row8 + number, blocks).astype(F32)

    def dense_rows(q, chunk, rows):
        held = jnp.broadcast_to(s.block_of[q, chunk : chunk + 1, :], (8, LANES))
        hits = {number: held == ids for number, ids in slab_ids.items()}
        result = []
        for slab in range(slabs):
            places = slab_rows[slab]
            value = jnp.broadcast_to(rows[places[0][0]], (8, LANES))
            if places[7][0] != places[0][0]:
                other = jnp.broadcast_to(rows[places[7][0]], (8, LANES))
                value = jnp.where(row8 < places.index((places[7][0], 0)), value, other)
            result.append(jnp.where(hits[places[0][1]], value, 0.0))
        return result

    def dense_spread(q, first, values):
        parts = [dense_rows(q, first + number, rows) for number, rows in enumerate(values)]
        parts += [[zero8] * slabs] * (4 - len(values))
        columns = [
            jnp.concatenate(parts[k] + parts[k + 2], axis=0).astype(BF16) for k in range(2)
        ]
        return jnp.concatenate(columns, axis=1)

    def spread(q, first, values):
        blank = jnp.zeros((half_rows, LANES), BF16)
        parts = []
        for number, value8 in enumerate(values):
            doubled = jnp.concatenate([value8, value8], axis=0).astype(BF16)
            held = s.block_of[q, first + number : first + number + 1, :]
            held = jnp.broadcast_to(held, (16, LANES)).astype(BF16)
            parts.append(
                jnp.concatenate(
                    [jnp.where(held == ids, doubled, zero16) for ids in block_ids], axis=0
                )
            )
        parts += [blank] * (4 - len(values))
        return jnp.concatenate(
            [jnp.concatenate(parts[0:2], axis=1), jnp.concatenate(parts[2:4], axis=1)], axis=0
        )

    def scattered(q, first, rows_from, get, count):
        total = None
        for at in range(0, count, 4):
            build = dense_spread if kind.dense else spread
            left = build(q, first + at, [get(k) for k in range(at, min(at + 4, count))])
            rows = slice(rows_from + at * 64, rows_from + at * 64 + 256)
            right = jnp.concatenate([s.onehot[q, half, rows, :] for half in range(2)], axis=1)
            term = jnp.dot(left, right, preferred_element_type=F32)
            total = term if total is None else total + term
        return total

    def fold(total, lane):
        if kind.dense:
            value = total[0:half_rows, 0:LANES] + total[half_rows:, LANES:]
            for c in range(3):
                at = (c + 3) * blocks
                whole = value[c * blocks : (c + 1) * blocks, :] + value[at : at + blocks, :]
                for copy in (0, 4):
                    at = (c + copy) * kind.blocks_pad
                    s.turn[lane, at : at + blocks, :] = whole
            return [
                s.turn[lane, pl.ds(block, 8, stride=kind.blocks_pad), :]
                for block in range(blocks)
            ]
        folded = []
        for block in range(blocks):
            rows = slice(block * 8, block * 8 + 8)
            other = slice(half_rows + block * 8, half_rows + block * 8 + 8)
            value = total[rows, 0:LANES] + total[other, LANES : 2 * LANES]
            folded.append(value + pltpu.roll(value, 4, 0))
        return folded

    def choose(found, bits):
        for bit in bits:
            found = [
                jnp.where(bit, found[k + 1], found[k]) if k + 1 < len(found) else found[k]
                for k in range(0, len(found), 2)
            ]
        return found[0]

    def bits_of(hi):
        count = (blocks - 1).bit_length()
        return [(hi & (1 << k)) != 0 for k in range(count)]

    def lookup(row, lo):
        return jnp.take_along_axis(row, lo, axis=1, mode="promise_in_bounds")

    def pick(source, lo, hi):
        found = [lookup(source(block), lo) for block in range(blocks)]
        return jnp.where(hi < 0, 0.0, choose(found, bits_of(hi)))

    def force(q, lane):
        stacked = []
        picked = {}
        for cut in range(cuts):
            groups = {c: [] for c in range(3)}
            for at in range(0, kind.points_pad, 8):
                lo = s.lo[q, cut, at : at + 8, :]
                bits = bits_of(s.hi[q, cut, at : at + 8, :])
                for c in range(3):
                    found = [
                        lookup(jnp.broadcast_to(s.now[q, block, c : c + 1, :], (8, LANES)), lo)
                        for block in range(blocks)
                    ]
                    groups[c].append(choose(found, bits))
            for c in range(3):
                picked[c, cut] = jnp.concatenate(groups[c], axis=0)
        order = [(c, cut) for c in range(3) for cut in range(cuts)]
        for key in order:
            high = high_part(picked[key])
            rows = [high, high, picked[key] - high]
            pad = kind.depth_in - 3 * kind.points_pad
            if pad:
                rows.append(jnp.zeros((pad, LANES), F32))
            stacked.append(jnp.concatenate(rows, axis=0).astype(BF16))
        grad = jnp.dot(
            lhs_in[...], jnp.concatenate(stacked, axis=1), preferred_element_type=F32
        )
        stacked = []
        for number, (c, cut) in enumerate(order):
            lanes = slice(number * LANES, (number + 1) * LANES)
            cut_lanes = slice(cut * LANES, (cut + 1) * LANES)
            pieces = [grad[b * quads_pad : (b + 1) * quads_pad, lanes] for b in range(3)]
            coef = [s.coefs[q, pair, :, cut_lanes] for pair in range(6)]
            flux = jnp.concatenate(
                [
                    coef[PAIR_OF[a, 0]] * pieces[0]
                    + coef[PAIR_OF[a, 1]] * pieces[1]
                    + coef[PAIR_OF[a, 2]] * pieces[2]
                    for a in range(3)
                ],
                axis=0,
            )
            high = high_part(flux)
            rows = [high, high, flux - high]
            pad = kind.depth_out - 9 * quads_pad
            if pad:
                rows.append(jnp.zeros((pad, LANES), F32))
            stacked.append(jnp.concatenate(rows, axis=0).astype(BF16))
        elem = jnp.dot(
            lhs_out[...], jnp.concatenate(stacked, axis=1), preferred_element_type=F32
        )
        for number, (c, cut) in enumerate(order):
            value = elem[:, number * LANES : (number + 1) * LANES]
            high = high_part(value)
            size = kind.points_pad
            s.parts[lane, cut, c * size : (c + 1) * size, :] = high
            at = (c + (3 if kind.dense else 4)) * size
            s.parts[lane, cut, at : at + size, :] = value - high
        def entry(chunk):
            cut, p = divmod(chunk, points)
            if kind.dense:
                rows = [part * kind.points_pad + p for part in range(6)]
                return [s.parts[lane, cut, row : row + 1, :] for row in rows]
            return s.parts[lane, cut, pl.ds(p, 8, stride=kind.points_pad), :]

        total = scattered(q, 0, 0, entry, kind.chunks)
        folded = fold(total, lane)
        for block in range(blocks):
            s.force[q, block] = folded[block]
        s.sends[q + 1] = pick(lambda block: folded[block], s.send_lo[q], s.send_hi[q])

    def split8(value):
        high = high_part(value)
        if kind.dense:
            return [part[c : c + 1, :] for part in (high, value - high) for c in range(3)]
        return jnp.where(low_half, high, value - high)

    def update(q, lane, step, forces, sends):
        lower = sends[q]
        upper = sends[q + 2]
        values = [
            jnp.where(low_half, pltpu.roll(lower, 4, 0), lower),
            jnp.where(low_half, upper, pltpu.roll(upper, 4, 0)),
        ]
        for m in range(kind.sources):
            four = layers[m][step, q]
            at = kind.at_layer + kind.sources + m
            values.append(jnp.concatenate([four, four], axis=0) * buf[q, at : at + 1, :])
        total = scattered(
            q, 4 * kind.tiles, main_rows, lambda k: split8(values[k]), len(values)
        )
        folded = fold(total, lane)
        after = []
        for block in range(blocks):
            now = s.now[q, block]
            scale = buf[q, kind.at_minv + block : kind.at_minv + block + 1, :]
            whole = forces[q, block] + folded[block]
            value = 2.0 * now - s.before[q, block] + scale * whole
            s.before[q, block] = now
            s.now[q, block] = value
            after.append(value)
        if emit is not None:
            picked = pick(lambda block: after[block], s.layer_lo[q], s.layer_hi[q])
            emit[step, q] = picked[0:4]

    def all_forces():
        def forces(group, _):
            for lane in range(unroll):
                force(group * unroll + lane, lane)
            return 0

        lax.fori_loop(0, width // unroll, forces, 0)

    def all_updates(step, forces, sends):
        def updates(group, _):
            for lane in range(unroll):
                update(group * unroll + lane, lane, step, forces, sends)
            return 0

        lax.fori_loop(0, width // unroll, updates, 0)

    def one_step(step, _):
        all_forces()
        all_updates(step, s.force, s.sends)
        return 0

    if mode == "first":
        all_forces()
        begun[0][...] = s.force[...]
        begun[1][...] = s.sends[...]
        return
    done = 0
    if mode == "rest":
        all_updates(0, *begun)
        done = 1
    lax.fori_loop(done, STEPS - 1, one_step, 0)
    span = min(4, unroll)
    first = jnp.clip(own - 1, 0, width - span)
    for lane in range(span):
        force(first + lane, lane)
    update(own, 0, STEPS - 1, s.force, s.sends)


SCRATCH = (
    "onehot", "block_of", "coefs", "lo", "hi", "send_lo", "send_hi", "layer_lo", "layer_hi",
    "now", "before", "force", "sends", "parts", "turn",
)


def scratch_of(kind, width, unroll):
    tiles = kind.tiles + kind.extra_tiles
    return [
        pltpu.VMEM((width, 2, tiles * 256, LANES), BF16),
        pltpu.VMEM((width, 4 * tiles, LANES), F32),
        pltpu.VMEM((width, 6, kind.quads_pad, kind.elems), F32),
        pltpu.VMEM((width, kind.cuts, kind.points_pad, LANES), jnp.int32),
        pltpu.VMEM((width, kind.cuts, kind.points_pad, LANES), jnp.int32),
        pltpu.VMEM((width, 8, LANES), jnp.int32),
        pltpu.VMEM((width, 8, LANES), jnp.int32),
        pltpu.VMEM((width, 8, LANES), jnp.int32),
        pltpu.VMEM((width, 8, LANES), jnp.int32),
        pltpu.VMEM((width, kind.blocks, 8, LANES), F32),
        pltpu.VMEM((width, kind.blocks, 8, LANES), F32),
        pltpu.VMEM((width, kind.blocks, 8, LANES), F32),
        pltpu.VMEM((width + 2, 8, LANES), F32),
        pltpu.VMEM((unroll, kind.cuts, 8 * kind.points_pad, LANES), F32),
        pltpu.VMEM((unroll, 8 * kind.blocks_pad, LANES), F32),
    ]


class Refs:
    pass


def window_base(index, count, width):
    return jnp.clip(index - STEPS, 0, count - width)


def sim_kernel(kind, width, unroll, offsets, mode, spare, *refs):
    sub = lax.axis_index("sub")
    count = lax.axis_size("sub")
    chips = count // 2
    bufs, refs = refs[:2], refs[2:]
    lhs_in, lhs_out, refs = refs[0], refs[1], refs[2:]
    layers = begun = emit = final = None
    if mode == "rest":
        layers, refs = refs[: kind.sources], refs[kind.sources :]
        begun, refs = refs[:2], refs[2:]
    if mode == "first":
        begun, refs = refs[:2], refs[2:]
    else:
        final, refs = refs[0], refs[1:]
    if mode == "all":
        emit, refs = refs[0], refs[1:]
    refs = refs[spare:]
    buf, sem, refs = refs[0], refs[1], refs[2:]
    s = Refs()
    for name, ref in zip(SCRATCH, refs, strict=True):
        setattr(s, name, ref)
    base = window_base(sub, count, width)
    if width < count:
        buf[...] = jnp.zeros(buf.shape, F32)
    copies = []
    for number, offset in enumerate(offsets):
        for other in range(2):
            chip = lax.rem(sub // 2 - offset + chips, chips)
            core = lax.rem(sub, 2)
            slot = chip * 2 + (core if other == 0 else 1 - core) - base
            at = 2 * number + other
            inside = jnp.logical_and(slot >= 0, slot < width)
            slot = jnp.clip(slot, 0, width - 1)
            copy = pltpu.make_async_copy(bufs[other].at[number], buf.at[slot], sem.at[at])
            copies.append((inside, copy))
    for phase in ("start", "wait"):
        for inside, copy in copies:
            if width < count:
                pl.when(inside)(getattr(copy, phase))
            else:
                getattr(copy, phase)()
    simulate(
        kind, width, unroll, sub - base, mode, buf, lhs_in, lhs_out, layers, emit, begun, s
    )
    if final is None:
        return
    for block in range(kind.blocks):
        for c in range(3):
            final[0, c, :, block * LANES : (block + 1) * LANES] = s.now[
                sub - base, block, c : c + 1, :
            ]


def begun_shapes(kind, width):
    return [
        jax.ShapeDtypeStruct((width, kind.blocks, 8, LANES), F32),
        jax.ShapeDtypeStruct((width + 2, 8, LANES), F32),
    ]


def layer_shape(width):
    return jax.ShapeDtypeStruct((STEPS, width, 4, LANES), F32)


def run_sim(kind, width, unroll, offsets, mode, bufs, tables, more, spare):
    if mode == "first":
        out_shape = begun_shapes(kind, width)
    else:
        out_shape = [jax.ShapeDtypeStruct((1, 3, 1, kind.count), F32)]
    if mode == "all":
        out_shape.append(layer_shape(width))
    vmem = pl.BlockSpec(memory_space=pltpu.VMEM)
    hbm = pl.BlockSpec(memory_space=pl.ANY)
    return pl.pallas_call(
        functools.partial(sim_kernel, kind, width, unroll, offsets, mode, len(spare)),
        out_shape=out_shape + spare,
        in_specs=[hbm] * len(bufs) + [vmem] * (2 + len(more)),
        out_specs=[vmem] * len(out_shape) + [hbm] * len(spare),
        scratch_shapes=[
            pltpu.VMEM((width, kind.rows, LANES), F32),
            pltpu.SemaphoreType.DMA((2 * len(offsets),)),
        ]
        + scratch_of(kind, width, unroll),
        name="sim_" + mode,
    )(*bufs, *tables, *more)


def blank_kernel(final, *rest):
    final[...] = jnp.zeros(final.shape, F32)


def gather_window(value, groups, offsets, count):
    chips = count // 2
    low, high = groups

    def moved(array, chip_shift, flip):
        route = []
        for grp in range(low, high):
            for index in range(count):
                chip, core = divmod(index, 2)
                target = ((chip + chip_shift) % chips) * 2 + (core ^ flip)
                route.append((grp * count + index, grp * count + target))
        return lax.ppermute(array, ("grp", "sub"), route)

    if len(offsets) == 1:
        joined = value[None]
        return [joined, moved(joined, 0, 1)]
    by_chip = [value if shift % chips == 0 else moved(value, shift, 0) for shift in offsets]
    joined = pl.pallas_call(
        join_kernel,
        out_shape=jax.ShapeDtypeStruct((len(offsets), *value.shape), F32),
        in_specs=[pl.BlockSpec(memory_space=pltpu.VMEM)] * len(offsets),
        out_specs=pl.BlockSpec(memory_space=pltpu.VMEM),
        name="join",
    )(*by_chip)
    return [joined, moved(joined, 0, 1)]


def join_kernel(*refs):
    for number, ref in enumerate(refs[:-1]):
        refs[-1][number] = ref[...]


def shards(
    reg_disp, reg_vel, site_disp, site_vel, reg_nodes, site_nodes, reg_coefs, site_coefs,
    reg_table, site_table, reg_minv, site_minv, reg_send, reg_recv, site_send, site_recv,
    slot_fill, layer_src, layer_fill, layer_dst, layer_stiff,
):
    group_count = lax.axis_size("grp")
    count = lax.axis_size("sub")
    site_groups = group_count // 4
    reg_groups = 3 * site_groups
    reg = Kind(reg_nodes, reg_coefs, reg_disp, 0)
    site = Kind(site_nodes, site_coefs, site_disp, 3)
    unroll = min(UNROLL, count)
    width = min(count, up_to(2 * STEPS + 1, unroll))
    chips = count // 2
    reach = STEPS // 2
    if 2 * reach + 1 >= chips:
        offsets = tuple(range(chips))
    else:
        offsets = tuple(range(-reach, reach + 1))
    is_site = lax.axis_index("grp") >= reg_groups
    vmem = pl.BlockSpec(memory_space=pltpu.VMEM)
    hbm = pl.BlockSpec(memory_space=pl.ANY)
    site_spare = [jax.ShapeDtypeStruct((len(offsets), site.rows, LANES), F32)] * 2 + [
        jax.ShapeDtypeStruct((3 * site.quads_pad, site.depth_in), BF16),
        jax.ShapeDtypeStruct((site.points_pad, site.depth_out), BF16),
        *begun_shapes(site, width),
    ]

    def regional():
        buf, *tables = pack(
            reg, reg_disp, reg_vel, reg_nodes, reg_coefs, reg_minv, reg_send, reg_recv,
            slot_fill, layer_src, layer_fill, reg_table,
        )
        bufs = gather_window(buf, (0, reg_groups), offsets, count)
        final, layer, *spare = run_sim(
            reg, width, unroll, offsets, "all", bufs, tables, (), site_spare
        )
        return (final, layer, *spare)

    def prepare_site():
        buf, *tables = pack(
            site, site_disp, site_vel, site_nodes, site_coefs, site_minv, site_send, site_recv,
            slot_fill, layer_dst, layer_stiff, site_table,
        )
        bufs = gather_window(buf, (reg_groups, group_count), offsets, count)
        final, layer = pl.pallas_call(
            blank_kernel,
            out_shape=[
                jax.ShapeDtypeStruct((1, 3, 1, reg.count), F32),
                layer_shape(width),
            ],
            out_specs=[vmem, hbm],
            name="blank",
        )()
        begun = run_sim(site, width, unroll, offsets, "first", bufs, tables, (), [])
        return (final, layer, *bufs, *tables, *begun)

    reg_final, layer_out, *rest = lax.cond(is_site, prepare_site, regional)
    site_bufs, site_tables, begun = rest[:2], rest[2:4], rest[4:]
    layers = [
        lax.ppermute(
            layer_out,
            "grp",
            [(m * site_groups + i, reg_groups + i) for i in range(site_groups)],
        )
        for m in range(3)
    ]

    def run_site():
        more = (*layers, *begun)
        return run_sim(site, width, unroll, offsets, "rest", site_bufs, site_tables, more, [])[0]

    def no_site():
        return jnp.zeros((1, 3, 1, site.count), F32)

    site_final = lax.cond(is_site, run_site, no_site)
    return jnp.transpose(reg_final, (0, 2, 1, 3)), jnp.transpose(site_final, (0, 2, 1, 3))


def solution(mesh):
    def spec(rank):
        return P("grp", "sub", *([None] * (rank - 2)))

    ranks = (4, 4, 4, 4, 4, 4, 6, 6, 0, 0, 3, 3, 4, 4, 4, 4, 3, 3, 2, 4, 4)
    return jax.shard_map(
        shards,
        mesh=mesh,
        in_specs=tuple(spec(rank) if rank else P() for rank in ranks),
        out_specs=(spec(4), spec(4)),
        check_vma=False,
    )
```

```python
import functools

import jax
import jax.numpy as jnp
from jax import lax
from jax.experimental import pallas as pl
from jax.experimental.pallas import tpu as pltpu
from jax.sharding import PartitionSpec as P

STEPS = 8
UNROLL = 8
LANES = 128
F32 = jnp.float32
BF16 = jnp.bfloat16
PAIRS = ((0, 0), (0, 1), (0, 2), (1, 1), (1, 2), (2, 2))
PAIR_OF = {**{ab: i for i, ab in enumerate(PAIRS)}, **{ab[::-1]: i for i, ab in enumerate(PAIRS)}}


def up_to(value, unit):
    return -(-value // unit) * unit


class Kind:
    def __init__(self, nodes, coefs, disp, sources):
        self.points, self.elems = nodes.shape[-2:]
        self.quads = coefs.shape[-2]
        self.count = disp.shape[-1]
        self.blocks = self.count // LANES
        self.cuts = self.elems // LANES
        self.points_pad = up_to(self.points, 8)
        self.quads_pad = up_to(self.quads, 8)
        self.blocks_pad = up_to(self.blocks, 2)
        self.depth_in = up_to(3 * self.points_pad, 16)
        self.depth_out = up_to(9 * self.quads_pad, 16)
        self.chunks = self.points * self.cuts
        self.sources = sources
        self.dense = self.blocks >= 8 and self.blocks % 4 == 0
        self.tiles = up_to(self.chunks, 4) // 4
        self.extra = 2 + sources
        self.extra_tiles = up_to(self.extra, 4) // 4
        self.table_turned = self.quads_pad == self.quads
        row = 0
        for name, rows in (
            ("coefs", 6 * self.quads * self.cuts),
            ("nodes", self.points * self.cuts),
            ("disp", 3 * self.blocks),
            ("vel", 3 * self.blocks),
            ("minv", self.blocks),
            ("send", 2),
            ("recv", 2),
            ("layer", 2 * sources if sources else 1),
        ):
            setattr(self, "at_" + name, row)
            row += rows
        self.rows = up_to(row, 8)


def pack_kernel(kind, *refs):
    inputs, refs = refs[:11], refs[11:]
    outputs, work, held, sem = refs[:3], refs[3], refs[4:15], refs[15]
    copies = [
        pltpu.make_async_copy(source, target, sem.at[number])
        for number, (source, target) in enumerate(zip(inputs, held, strict=True))
    ]
    for copy in copies:
        copy.start()
    work[...] = jnp.zeros(work.shape, F32)
    for copy in copies:
        copy.wait()
    fill_packed(kind, *held, *outputs, work)


def fill_packed(kind, *refs):
    disp, vel, nodes, coefs, minv, send, recv, fill, layer_a, layer_b, table, out, first, second = refs[:14]
    work = refs[14]
    for pair, (a, b) in enumerate(PAIRS):
        for cut in range(kind.cuts):
            at = kind.at_coefs + (pair * kind.cuts + cut) * kind.quads
            out[at : at + kind.quads, :] = coefs[0, 0, a, b, :, cut * LANES : (cut + 1) * LANES]
    for cut in range(kind.cuts):
        for p in range(kind.points):
            at = kind.at_nodes + cut * kind.points + p
            out[at : at + 1, :] = nodes[0, p, :, cut * LANES : (cut + 1) * LANES].astype(F32)
    for block in range(kind.blocks):
        lanes = slice(block * LANES, (block + 1) * LANES)
        for c in range(3):
            for at, ref in ((kind.at_disp, disp), (kind.at_vel, vel)):
                out[at + 3 * block + c : at + 3 * block + c + 1, :] = ref[0, c, :, lanes]
        out[kind.at_minv + block : kind.at_minv + block + 1, :] = minv[0, 0:1, lanes]
    lane = lax.broadcasted_iota(jnp.int32, (1, LANES), 1)
    for side in range(2):
        at = (2 if kind.sources else 0) + side
        live = lane < jnp.broadcast_to(fill[0, 0:1, at : at + 1], (1, LANES))
        row = send[0, 0, side : side + 1, :]
        out[kind.at_send + side : kind.at_send + side + 1, :] = jnp.where(live, row, -1).astype(F32)
    out[kind.at_recv : kind.at_recv + 2, :] = recv[0, 0].astype(F32)
    for m in range(kind.sources):
        at = kind.at_layer + m
        out[at : at + 1, :] = layer_a[0, m].astype(F32)
        out[at + kind.sources : at + kind.sources + 1, :] = layer_b[0, m]
    if not kind.sources:
        row = layer_a[0, 0:1, :]
        live = lane < jnp.broadcast_to(layer_b[0:1, 0:1], (1, LANES))
        out[kind.at_layer : kind.at_layer + 1, :] = jnp.where(live, row, -1).astype(F32)
    size = kind.quads_pad
    if kind.table_turned:
        work[0 : kind.points, 0 : 3 * kind.quads] = table[...]
        turned = work[...]
        plain = jnp.transpose(turned)
    else:
        for a in range(3):
            work[a * size : a * size + kind.quads, 0 : kind.points] = table[
                a * kind.quads : (a + 1) * kind.quads, :
            ]
        plain = work[...]
        turned = jnp.transpose(plain)
    step = kind.points_pad
    high = high_part(plain)
    low = plain - high
    rows = high + pltpu.roll(low, step, 1) + pltpu.roll(high, 2 * step, 1)
    first[...] = rows[0 : 3 * size, 0 : kind.depth_in].astype(BF16)
    high = high_part(turned)
    low = turned - high
    wide = jnp.zeros((LANES, LANES), F32)
    high = jnp.concatenate([high, wide], axis=1)
    low = jnp.concatenate([low, wide], axis=1)
    rows = high + pltpu.roll(low, 3 * size, 1) + pltpu.roll(high, 6 * size, 1)
    second[...] = (-rows[0 : kind.points_pad, 0 : kind.depth_out]).astype(BF16)


def pack(kind, disp, vel, nodes, coefs, minv, send, recv, fill, layer_a, layer_b, table):
    def thin(array):
        return jnp.transpose(array, (0, 2, 1, 3))

    vmem = pl.BlockSpec(memory_space=pltpu.VMEM)
    hbm = pl.BlockSpec(memory_space=pl.ANY)
    if kind.sources:
        layer_a, layer_b = thin(layer_a), thin(layer_b)
    if kind.table_turned:
        table = table.T
    inputs = (
        thin(disp), thin(vel), thin(nodes), coefs, minv, send, recv, fill, layer_a, layer_b, table,
    )
    return pl.pallas_call(
        functools.partial(pack_kernel, kind),
        out_shape=[
            jax.ShapeDtypeStruct((kind.rows, LANES), F32),
            jax.ShapeDtypeStruct((3 * kind.quads_pad, kind.depth_in), BF16),
            jax.ShapeDtypeStruct((kind.points_pad, kind.depth_out), BF16),
        ],
        in_specs=[hbm] * len(inputs),
        out_specs=[vmem] * 3,
        scratch_shapes=[
            pltpu.VMEM((LANES, LANES), F32),
            *[pltpu.VMEM(array.shape, array.dtype) for array in inputs],
            pltpu.SemaphoreType.DMA((len(inputs),)),
        ],
        name="site_pack" if kind.sources else "reg_pack",
    )(*inputs)


def split_index(value):
    index = value.astype(jnp.int32)
    return index & (LANES - 1), index >> 7


def high_part(value):
    return value.astype(BF16).astype(F32)


def simulate(kind, width, unroll, own, mode, buf, lhs_in, lhs_out, layers, emit, begun, s):
    points, cuts, blocks = kind.points, kind.cuts, kind.blocks
    quads_pad = kind.quads_pad
    half_rows = 6 * blocks if kind.dense else 8 * kind.blocks_pad
    row8 = lax.broadcasted_iota(jnp.int32, (8, LANES), 0)
    low_half = row8 < 4
    row16 = lax.broadcasted_iota(jnp.int32, (16, LANES), 0)
    block_ids = [
        jnp.where(row16 < 8, 2 * j, 2 * j + 1).astype(F32).astype(BF16)
        for j in range(kind.blocks_pad // 2)
    ]
    zero16 = jnp.zeros((16, LANES), BF16)
    zero8 = jnp.zeros((8, LANES), F32)
    lane_ids = lax.broadcasted_iota(jnp.int32, (LANES, LANES), 1).astype(F32).astype(BF16)
    one = jnp.ones((LANES, LANES), BF16)
    none = jnp.zeros((LANES, LANES), BF16)
    main_rows = kind.tiles * 256

    def onehot(q, chunk_no, base_row, columns, at):
        hit = columns[:, at : at + 1] == lane_ids
        tile, half, part = chunk_no // 4, (chunk_no // 2) % 2, chunk_no % 2
        rows = pl.ds(base_row + tile * 256 + part * LANES, LANES)
        s.onehot[q, half, rows, :] = jnp.where(hit, one, none)

    def hold_block(q, chunk_no, hi_row):
        s.block_of[q, chunk_no : chunk_no + 1, :] = hi_row.astype(F32)

    def columns_of(rows):
        count = rows.shape[0]
        if count < LANES:
            rows = jnp.concatenate([rows, jnp.zeros((LANES - count, LANES), F32)], axis=0)
        return jnp.transpose(rows).astype(BF16)

    def setup(q, _):
        for pair in range(6):
            for cut in range(cuts):
                at = kind.at_coefs + (pair * cuts + cut) * kind.quads
                lanes = slice(cut * LANES, (cut + 1) * LANES)
                if kind.quads_pad > kind.quads:
                    s.coefs[q, pair, :, lanes] = jnp.zeros((quads_pad, LANES), F32)
                s.coefs[q, pair, 0 : kind.quads, lanes] = buf[q, at : at + kind.quads, :]
        for cut in range(cuts):
            at = kind.at_nodes + cut * points
            value = buf[q, at : at + points, :]
            lo, hi = split_index(value)
            if kind.points_pad > points:
                s.lo[q, cut] = jnp.zeros((kind.points_pad, LANES), jnp.int32)
                s.hi[q, cut] = jnp.zeros((kind.points_pad, LANES), jnp.int32)
            s.lo[q, cut, 0:points, :] = lo
            s.hi[q, cut, 0:points, :] = hi
            columns = columns_of(lo.astype(F32))
            for p in range(points):
                onehot(q, cut * points + p, 0, columns, p)
                hold_block(q, cut * points + p, hi[p : p + 1, :])
        for chunk in range(kind.chunks, 4 * kind.tiles):
            columns = jnp.zeros((LANES, LANES), BF16)
            onehot(q, chunk, 0, columns, 0)
            hold_block(q, chunk, jnp.zeros((1, LANES), jnp.int32))
        extra = [buf[q, kind.at_recv : kind.at_recv + 2, :]]
        if kind.sources:
            extra.append(buf[q, kind.at_layer : kind.at_layer + kind.sources, :])
        extra.append(jnp.zeros((4 * kind.extra_tiles - kind.extra, LANES), F32))
        lo, hi = split_index(jnp.concatenate([e for e in extra if e.shape[0]], axis=0))
        columns = columns_of(lo.astype(F32))
        for chunk in range(4 * kind.extra_tiles):
            onehot(q, chunk, main_rows, columns, chunk)
            hold_block(q, 4 * kind.tiles + chunk, hi[chunk : chunk + 1, :])
        send_rows = [
            jnp.broadcast_to(buf[q, kind.at_send + side : kind.at_send + side + 1, :], (4, LANES))
            for side in range(2)
        ]
        s.send_lo[q], s.send_hi[q] = split_index(jnp.concatenate(send_rows, axis=0))
        if not kind.sources:
            row = buf[q, kind.at_layer : kind.at_layer + 1, :]
            s.layer_lo[q], s.layer_hi[q] = split_index(jnp.broadcast_to(row, (8, LANES)))
        for block in range(blocks):
            at = kind.at_disp + 3 * block
            now = buf[q, at : at + 3, :]
            at = kind.at_vel + 3 * block
            before = now - buf[q, at : at + 3, :]
            for ref, value in ((s.now, now), (s.before, before)):
                ref[q, block] = zero8
                ref[q, block, 0:3, :] = value
                ref[q, block, 4:7, :] = value
        return 0

    def setup_pair(pair, _):
        for k in range(2):
            setup(2 * pair + k, 0)
        return 0

    lax.fori_loop(0, width // 2, setup_pair, 0)
    for lane in range(unroll):
        s.parts[lane] = jnp.zeros(s.parts.shape[1:], F32)
        s.turn[lane] = jnp.zeros(s.turn.shape[1:], F32)
    s.sends[0] = zero8
    s.sends[width + 1] = zero8

    slabs = half_rows // 8
    slab_rows = [
        [divmod(8 * slab + row, blocks) for row in range(8)] for slab in range(slabs)
    ]
    slab_ids = {}
    for slab in range(slabs if kind.dense else 0):
        number = slab_rows[slab][0][1]
        if number not in slab_ids:
            slab_ids[number] = lax.rem(row8 + number, blocks).astype(F32)

    def dense_rows(q, chunk, rows):
        held = jnp.broadcast_to(s.block_of[q, chunk : chunk + 1, :], (8, LANES))
        hits = {number: held == ids for number, ids in slab_ids.items()}
        result = []
        for slab in range(slabs):
            places = slab_rows[slab]
            value = jnp.broadcast_to(rows[places[0][0]], (8, LANES))
            if places[7][0] != places[0][0]:
                other = jnp.broadcast_to(rows[places[7][0]], (8, LANES))
                value = jnp.where(row8 < places.index((places[7][0], 0)), value, other)
            result.append(jnp.where(hits[places[0][1]], value, 0.0))
        return result

    def dense_spread(q, first, values):
        parts = [dense_rows(q, first + number, rows) for number, rows in enumerate(values)]
        parts += [[zero8] * slabs] * (4 - len(values))
        columns = [
            jnp.concatenate(parts[k] + parts[k + 2], axis=0).astype(BF16) for k in range(2)
        ]
        return jnp.concatenate(columns, axis=1)

    def spread(q, first, values):
        blank = jnp.zeros((half_rows, LANES), BF16)
        parts = []
        for number, value8 in enumerate(values):
            doubled = jnp.concatenate([value8, value8], axis=0).astype(BF16)
            held = s.block_of[q, first + number : first + number + 1, :]
            held = jnp.broadcast_to(held, (16, LANES)).astype(BF16)
            parts.append(
                jnp.concatenate(
                    [jnp.where(held == ids, doubled, zero16) for ids in block_ids], axis=0
                )
            )
        parts += [blank] * (4 - len(values))
        return jnp.concatenate(
            [jnp.concatenate(parts[0:2], axis=1), jnp.concatenate(parts[2:4], axis=1)], axis=0
        )

    def scattered(q, first, rows_from, get, count):
        total = None
        for at in range(0, count, 4):
            build = dense_spread if kind.dense else spread
            left = build(q, first + at, [get(k) for k in range(at, min(at + 4, count))])
            rows = slice(rows_from + at * 64, rows_from + at * 64 + 256)
            right = jnp.concatenate([s.onehot[q, half, rows, :] for half in range(2)], axis=1)
            term = jnp.dot(left, right, preferred_element_type=F32)
            total = term if total is None else total + term
        return total

    def fold(total, lane):
        if kind.dense:
            value = total[0:half_rows, 0:LANES] + total[half_rows:, LANES:]
            for c in range(3):
                at = (c + 3) * blocks
                whole = value[c * blocks : (c + 1) * blocks, :] + value[at : at + blocks, :]
                for copy in (0, 4):
                    at = (c + copy) * kind.blocks_pad
                    s.turn[lane, at : at + blocks, :] = whole
            return [
                s.turn[lane, pl.ds(block, 8, stride=kind.blocks_pad), :]
                for block in range(blocks)
            ]
        folded = []
        for block in range(blocks):
            rows = slice(block * 8, block * 8 + 8)
            other = slice(half_rows + block * 8, half_rows + block * 8 + 8)
            value = total[rows, 0:LANES] + total[other, LANES : 2 * LANES]
            folded.append(value + pltpu.roll(value, 4, 0))
        return folded

    def choose(found, bits):
        for bit in bits:
            found = [
                jnp.where(bit, found[k + 1], found[k]) if k + 1 < len(found) else found[k]
                for k in range(0, len(found), 2)
            ]
        return found[0]

    def bits_of(hi):
        count = (blocks - 1).bit_length()
        return [(hi & (1 << k)) != 0 for k in range(count)]

    def lookup(row, lo):
        return jnp.take_along_axis(row, lo, axis=1, mode="promise_in_bounds")

    def pick(source, lo, hi):
        found = [lookup(source(block), lo) for block in range(blocks)]
        return jnp.where(hi < 0, 0.0, choose(found, bits_of(hi)))

    def force(q, lane):
        stacked = []
        picked = {}
        for cut in range(cuts):
            groups = {c: [] for c in range(3)}
            for at in range(0, kind.points_pad, 8):
                lo = s.lo[q, cut, at : at + 8, :]
                bits = bits_of(s.hi[q, cut, at : at + 8, :])
                for c in range(3):
                    found = [
                        lookup(jnp.broadcast_to(s.now[q, block, c : c + 1, :], (8, LANES)), lo)
                        for block in range(blocks)
                    ]
                    groups[c].append(choose(found, bits))
            for c in range(3):
                picked[c, cut] = jnp.concatenate(groups[c], axis=0)
        order = [(c, cut) for c in range(3) for cut in range(cuts)]
        for key in order:
            high = high_part(picked[key])
            rows = [high, high, picked[key] - high]
            pad = kind.depth_in - 3 * kind.points_pad
            if pad:
                rows.append(jnp.zeros((pad, LANES), F32))
            stacked.append(jnp.concatenate(rows, axis=0).astype(BF16))
        grad = jnp.dot(
            lhs_in[...], jnp.concatenate(stacked, axis=1), preferred_element_type=F32
        )
        stacked = []
        for number, (c, cut) in enumerate(order):
            lanes = slice(number * LANES, (number + 1) * LANES)
            cut_lanes = slice(cut * LANES, (cut + 1) * LANES)
            pieces = [grad[b * quads_pad : (b + 1) * quads_pad, lanes] for b in range(3)]
            coef = [s.coefs[q, pair, :, cut_lanes] for pair in range(6)]
            flux = jnp.concatenate(
                [
                    coef[PAIR_OF[a, 0]] * pieces[0]
                    + coef[PAIR_OF[a, 1]] * pieces[1]
                    + coef[PAIR_OF[a, 2]] * pieces[2]
                    for a in range(3)
                ],
                axis=0,
            )
            high = high_part(flux)
            rows = [high, high, flux - high]
            pad = kind.depth_out - 9 * quads_pad
            if pad:
                rows.append(jnp.zeros((pad, LANES), F32))
            stacked.append(jnp.concatenate(rows, axis=0).astype(BF16))
        elem = jnp.dot(
            lhs_out[...], jnp.concatenate(stacked, axis=1), preferred_element_type=F32
        )
        for number, (c, cut) in enumerate(order):
            value = elem[:, number * LANES : (number + 1) * LANES]
            high = high_part(value)
            size = kind.points_pad
            s.parts[lane, cut, c * size : (c + 1) * size, :] = high
            at = (c + (3 if kind.dense else 4)) * size
            s.parts[lane, cut, at : at + size, :] = value - high
        def entry(chunk):
            cut, p = divmod(chunk, points)
            if kind.dense:
                rows = [part * kind.points_pad + p for part in range(6)]
                return [s.parts[lane, cut, row : row + 1, :] for row in rows]
            return s.parts[lane, cut, pl.ds(p, 8, stride=kind.points_pad), :]

        total = scattered(q, 0, 0, entry, kind.chunks)
        folded = fold(total, lane)
        for block in range(blocks):
            s.force[q, block] = folded[block]
        s.sends[q + 1] = pick(lambda block: folded[block], s.send_lo[q], s.send_hi[q])

    def split8(value):
        high = high_part(value)
        if kind.dense:
            return [part[c : c + 1, :] for part in (high, value - high) for c in range(3)]
        return jnp.where(low_half, high, value - high)

    def update(q, lane, step, forces, sends):
        lower = sends[q]
        upper = sends[q + 2]
        values = [
            jnp.where(low_half, pltpu.roll(lower, 4, 0), lower),
            jnp.where(low_half, upper, pltpu.roll(upper, 4, 0)),
        ]
        for m in range(kind.sources):
            at = kind.at_layer + kind.sources + m
            rows = [layers[m][step, c, pl.ds(q, 1), :] for c in range(3)]
            rows = jnp.concatenate([*rows, jnp.zeros((1, LANES), F32)] * 2, axis=0)
            values.append(rows * buf[q, at : at + 1, :])
        total = scattered(
            q, 4 * kind.tiles, main_rows, lambda k: split8(values[k]), len(values)
        )
        folded = fold(total, lane)
        after = []
        for block in range(blocks):
            now = s.now[q, block]
            scale = buf[q, kind.at_minv + block : kind.at_minv + block + 1, :]
            whole = forces[q, block] + folded[block]
            value = 2.0 * now - s.before[q, block] + scale * whole
            s.before[q, block] = now
            s.now[q, block] = value
            after.append(value)
        if emit is not None:
            picked = pick(lambda block: after[block], s.layer_lo[q], s.layer_hi[q])
            for c in range(3):
                emit[step, c, pl.ds(q, 1), :] = picked[c : c + 1, :]

    def all_forces():
        def forces(group, _):
            for lane in range(unroll):
                force(group * unroll + lane, lane)
            return 0

        lax.fori_loop(0, width // unroll, forces, 0)

    def all_updates(step, forces, sends):
        def updates(group, _):
            for lane in range(unroll):
                update(group * unroll + lane, lane, step, forces, sends)
            return 0

        lax.fori_loop(0, width // unroll, updates, 0)

    def one_step(step, _):
        all_forces()
        all_updates(step, s.force, s.sends)
        return 0

    if mode == "first":
        all_forces()
        begun[0][...] = s.force[...]
        begun[1][...] = s.sends[...]
        return
    done = 0
    if mode == "rest":
        all_updates(0, *begun)
        done = 1
    tail = max(done, STEPS - 2)
    lax.fori_loop(done, tail, one_step, 0)
    for step in range(tail, STEPS):
        reach = STEPS - step
        for span, run in (
            (min(2 * reach + 1, width), force),
            (min(2 * reach - 1, width), functools.partial(update, step=step, forces=s.force, sends=s.sends)),
        ):
            first = jnp.clip(own - span // 2, 0, width - span)
            for lane in range(span):
                run(first + lane, lane % unroll)


SCRATCH = (
    "onehot", "block_of", "coefs", "lo", "hi", "send_lo", "send_hi", "layer_lo", "layer_hi",
    "now", "before", "force", "sends", "parts", "turn",
)


def scratch_of(kind, width, unroll):
    tiles = kind.tiles + kind.extra_tiles
    return [
        pltpu.VMEM((width, 2, tiles * 256, LANES), BF16),
        pltpu.VMEM((width, 4 * tiles, LANES), F32),
        pltpu.VMEM((width, 6, kind.quads_pad, kind.elems), F32),
        pltpu.VMEM((width, kind.cuts, kind.points_pad, LANES), jnp.int32),
        pltpu.VMEM((width, kind.cuts, kind.points_pad, LANES), jnp.int32),
        pltpu.VMEM((width, 8, LANES), jnp.int32),
        pltpu.VMEM((width, 8, LANES), jnp.int32),
        pltpu.VMEM((width, 8, LANES), jnp.int32),
        pltpu.VMEM((width, 8, LANES), jnp.int32),
        pltpu.VMEM((width, kind.blocks, 8, LANES), F32),
        pltpu.VMEM((width, kind.blocks, 8, LANES), F32),
        pltpu.VMEM((width, kind.blocks, 8, LANES), F32),
        pltpu.VMEM((width + 2, 8, LANES), F32),
        pltpu.VMEM((unroll, kind.cuts, 8 * kind.points_pad, LANES), F32),
        pltpu.VMEM((unroll, 8 * kind.blocks_pad, LANES), F32),
    ]


class Refs:
    pass


def window_base(index, count, width):
    return jnp.clip(index - STEPS, 0, count - width)


def sim_kernel(kind, width, unroll, offsets, mode, spare, *refs):
    sub = lax.axis_index("sub")
    count = lax.axis_size("sub")
    chips = count // 2
    bufs, refs = refs[:2], refs[2:]
    lhs_in, lhs_out, refs = refs[0], refs[1], refs[2:]
    layers = begun = emit = final = None
    if mode == "rest":
        layers, refs = refs[: kind.sources], refs[kind.sources :]
        begun, refs = refs[:2], refs[2:]
    if mode == "first":
        begun, refs = refs[:2], refs[2:]
    else:
        final, refs = refs[0], refs[1:]
    if mode == "all":
        emit, refs = refs[0], refs[1:]
    refs = refs[spare:]
    buf, sem, refs = refs[0], refs[1], refs[2:]
    s = Refs()
    for name, ref in zip(SCRATCH, refs, strict=True):
        setattr(s, name, ref)
    base = window_base(sub, count, width)
    if width < count:
        buf[...] = jnp.zeros(buf.shape, F32)
    copies = []
    for number, offset in enumerate(offsets):
        for other in range(2):
            chip = lax.rem(sub // 2 - offset + chips, chips)
            core = lax.rem(sub, 2)
            slot = chip * 2 + (core if other == 0 else 1 - core) - base
            at = 2 * number + other
            inside = jnp.logical_and(slot >= 0, slot < width)
            slot = jnp.clip(slot, 0, width - 1)
            copy = pltpu.make_async_copy(bufs[other].at[number], buf.at[slot], sem.at[at])
            copies.append((inside, copy))
    for phase in ("start", "wait"):
        for inside, copy in copies:
            if width < count:
                pl.when(inside)(getattr(copy, phase))
            else:
                getattr(copy, phase)()
    simulate(
        kind, width, unroll, sub - base, mode, buf, lhs_in, lhs_out, layers, emit, begun, s
    )
    if final is None:
        return
    for block in range(kind.blocks):
        for c in range(3):
            final[0, c, :, block * LANES : (block + 1) * LANES] = s.now[
                sub - base, block, c : c + 1, :
            ]


def begun_shapes(kind, width):
    return [
        jax.ShapeDtypeStruct((width, kind.blocks, 8, LANES), F32),
        jax.ShapeDtypeStruct((width + 2, 8, LANES), F32),
    ]


def layer_shape(width):
    return jax.ShapeDtypeStruct((STEPS, 3, width, LANES), F32)


def run_sim(kind, width, unroll, offsets, mode, bufs, tables, more, spare):
    if mode == "first":
        out_shape = begun_shapes(kind, width)
    else:
        out_shape = [jax.ShapeDtypeStruct((1, 3, 1, kind.count), F32)]
    if mode == "all":
        out_shape.append(layer_shape(width))
    vmem = pl.BlockSpec(memory_space=pltpu.VMEM)
    hbm = pl.BlockSpec(memory_space=pl.ANY)
    return pl.pallas_call(
        functools.partial(sim_kernel, kind, width, unroll, offsets, mode, len(spare)),
        out_shape=out_shape + spare,
        in_specs=[hbm] * len(bufs) + [vmem] * (2 + len(more)),
        out_specs=[vmem] * len(out_shape) + [hbm] * len(spare),
        scratch_shapes=[
            pltpu.VMEM((width, kind.rows, LANES), F32),
            pltpu.SemaphoreType.DMA((2 * len(offsets),)),
        ]
        + scratch_of(kind, width, unroll),
        name="sim_" + mode,
    )(*bufs, *tables, *more)


def blank_kernel(final, *rest):
    final[...] = jnp.zeros(final.shape, F32)


def gather_window(value, groups, offsets, count):
    chips = count // 2
    low, high = groups

    def moved(array, chip_shift, flip):
        route = []
        for grp in range(low, high):
            for index in range(count):
                chip, core = divmod(index, 2)
                target = ((chip + chip_shift) % chips) * 2 + (core ^ flip)
                route.append((grp * count + index, grp * count + target))
        return lax.ppermute(array, ("grp", "sub"), route)

    if len(offsets) == 1:
        joined = value[None]
        return [joined, moved(joined, 0, 1)]
    by_chip = [value if shift % chips == 0 else moved(value, shift, 0) for shift in offsets]
    joined = pl.pallas_call(
        join_kernel,
        out_shape=jax.ShapeDtypeStruct((len(offsets), *value.shape), F32),
        in_specs=[pl.BlockSpec(memory_space=pltpu.VMEM)] * len(offsets),
        out_specs=pl.BlockSpec(memory_space=pltpu.VMEM),
        name="join",
    )(*by_chip)
    return [joined, moved(joined, 0, 1)]


def join_kernel(*refs):
    for number, ref in enumerate(refs[:-1]):
        refs[-1][number] = ref[...]


def shards(
    reg_disp, reg_vel, site_disp, site_vel, reg_nodes, site_nodes, reg_coefs, site_coefs,
    reg_table, site_table, reg_minv, site_minv, reg_send, reg_recv, site_send, site_recv,
    slot_fill, layer_src, layer_fill, layer_dst, layer_stiff,
):
    group_count = lax.axis_size("grp")
    count = lax.axis_size("sub")
    site_groups = group_count // 4
    reg_groups = 3 * site_groups
    reg = Kind(reg_nodes, reg_coefs, reg_disp, 0)
    site = Kind(site_nodes, site_coefs, site_disp, 3)
    unroll = min(UNROLL, count)
    width = min(count, up_to(2 * STEPS + 1, unroll))
    chips = count // 2
    reach = STEPS // 2
    if 2 * reach + 1 >= chips:
        offsets = tuple(range(chips))
    else:
        offsets = tuple(range(-reach, reach + 1))
    is_site = lax.axis_index("grp") >= reg_groups
    vmem = pl.BlockSpec(memory_space=pltpu.VMEM)
    hbm = pl.BlockSpec(memory_space=pl.ANY)
    site_spare = [jax.ShapeDtypeStruct((len(offsets), site.rows, LANES), F32)] * 2 + [
        jax.ShapeDtypeStruct((3 * site.quads_pad, site.depth_in), BF16),
        jax.ShapeDtypeStruct((site.points_pad, site.depth_out), BF16),
        *begun_shapes(site, width),
    ]

    def regional():
        buf, *tables = pack(
            reg, reg_disp, reg_vel, reg_nodes, reg_coefs, reg_minv, reg_send, reg_recv,
            slot_fill, layer_src, layer_fill, reg_table,
        )
        bufs = gather_window(buf, (0, reg_groups), offsets, count)
        final, layer, *spare = run_sim(
            reg, width, unroll, offsets, "all", bufs, tables, (), site_spare
        )
        return (final, layer, *spare)

    def prepare_site():
        buf, *tables = pack(
            site, site_disp, site_vel, site_nodes, site_coefs, site_minv, site_send, site_recv,
            slot_fill, layer_dst, layer_stiff, site_table,
        )
        bufs = gather_window(buf, (reg_groups, group_count), offsets, count)
        final, layer = pl.pallas_call(
            blank_kernel,
            out_shape=[
                jax.ShapeDtypeStruct((1, 3, 1, reg.count), F32),
                layer_shape(width),
            ],
            out_specs=[vmem, hbm],
            name="blank",
        )()
        begun = run_sim(site, width, unroll, offsets, "first", bufs, tables, (), [])
        return (final, layer, *bufs, *tables, *begun)

    reg_final, layer_out, *rest = lax.cond(is_site, prepare_site, regional)
    site_bufs, site_tables, begun = rest[:2], rest[2:4], rest[4:]
    layers = [
        lax.ppermute(
            layer_out,
            "grp",
            [(m * site_groups + i, reg_groups + i) for i in range(site_groups)],
        )
        for m in range(3)
    ]

    def run_site():
        more = (*layers, *begun)
        return run_sim(site, width, unroll, offsets, "rest", site_bufs, site_tables, more, [])[0]

    def no_site():
        return jnp.zeros((1, 3, 1, site.count), F32)

    site_final = lax.cond(is_site, run_site, no_site)
    return jnp.transpose(reg_final, (0, 2, 1, 3)), jnp.transpose(site_final, (0, 2, 1, 3))


def solution(mesh):
    def spec(rank):
        return P("grp", "sub", *([None] * (rank - 2)))

    ranks = (4, 4, 4, 4, 4, 4, 6, 6, 0, 0, 3, 3, 4, 4, 4, 4, 3, 3, 2, 4, 4)
    return jax.shard_map(
        shards,
        mesh=mesh,
        in_specs=tuple(spec(rank) if rank else P() for rank in ranks),
        out_specs=(spec(4), spec(4)),
        check_vma=False,
    )
```

```python
import functools

import jax
import jax.numpy as jnp
from jax import lax
from jax.experimental import pallas as pl
from jax.experimental.pallas import tpu as pltpu
from jax.sharding import PartitionSpec as P

STEPS = 8
UNROLL = 8
LANES = 128
F32 = jnp.float32
BF16 = jnp.bfloat16
PAIRS = ((0, 0), (0, 1), (0, 2), (1, 1), (1, 2), (2, 2))
PAIR_OF = {**{ab: i for i, ab in enumerate(PAIRS)}, **{ab[::-1]: i for i, ab in enumerate(PAIRS)}}


def up_to(value, unit):
    return -(-value // unit) * unit


class Kind:
    def __init__(self, nodes, coefs, disp, sources):
        self.points, self.elems = nodes.shape[-2:]
        self.quads = coefs.shape[-2]
        self.count = disp.shape[-1]
        self.blocks = self.count // LANES
        self.cuts = self.elems // LANES
        self.points_pad = up_to(self.points, 8)
        self.quads_pad = up_to(self.quads, 8)
        self.blocks_pad = up_to(self.blocks, 2)
        self.depth_in = up_to(3 * self.points_pad, 16)
        self.depth_out = up_to(9 * self.quads_pad, 16)
        self.chunks = self.points * self.cuts
        self.sources = sources
        self.dense = self.blocks >= 8 and self.blocks % 4 == 0
        self.tiles = up_to(self.chunks, 4) // 4
        self.extra = 2 + sources
        self.extra_tiles = up_to(self.extra, 4) // 4
        self.table_turned = self.quads_pad == self.quads
        row = 0
        for name, rows in (
            ("coefs", 6 * self.quads * self.cuts),
            ("nodes", self.points * self.cuts),
            ("disp", 3 * self.blocks),
            ("vel", 3 * self.blocks),
            ("minv", self.blocks),
            ("send", 2),
            ("recv", 2),
            ("layer", 2 * sources if sources else 1),
        ):
            setattr(self, "at_" + name, row)
            row += rows
        self.rows = up_to(row, 8)


def pack_kernel(kind, *refs):
    inputs, refs = refs[:11], refs[11:]
    outputs, work, held, sem = refs[:3], refs[3], refs[4:15], refs[15]
    copies = [
        pltpu.make_async_copy(source, target, sem.at[number])
        for number, (source, target) in enumerate(zip(inputs, held, strict=True))
    ]
    for copy in copies:
        copy.start()
    work[...] = jnp.zeros(work.shape, F32)
    for copy in copies:
        copy.wait()
    fill_packed(kind, *held, *outputs, work)


def fill_packed(kind, *refs):
    disp, vel, nodes, coefs, minv, send, recv, fill, layer_a, layer_b, table, out, first, second = refs[:14]
    work = refs[14]
    for pair, (a, b) in enumerate(PAIRS):
        for cut in range(kind.cuts):
            at = kind.at_coefs + (pair * kind.cuts + cut) * kind.quads
            out[at : at + kind.quads, :] = coefs[0, 0, a, b, :, cut * LANES : (cut + 1) * LANES]
    for cut in range(kind.cuts):
        for p in range(kind.points):
            at = kind.at_nodes + cut * kind.points + p
            out[at : at + 1, :] = nodes[0, p, :, cut * LANES : (cut + 1) * LANES].astype(F32)
    for block in range(kind.blocks):
        lanes = slice(block * LANES, (block + 1) * LANES)
        for c in range(3):
            for at, ref in ((kind.at_disp, disp), (kind.at_vel, vel)):
                out[at + 3 * block + c : at + 3 * block + c + 1, :] = ref[0, c, :, lanes]
        out[kind.at_minv + block : kind.at_minv + block + 1, :] = minv[0, 0:1, lanes]
    lane = lax.broadcasted_iota(jnp.int32, (1, LANES), 1)
    for side in range(2):
        at = (2 if kind.sources else 0) + side
        live = lane < jnp.broadcast_to(fill[0, 0:1, at : at + 1], (1, LANES))
        row = send[0, 0, side : side + 1, :]
        out[kind.at_send + side : kind.at_send + side + 1, :] = jnp.where(live, row, -1).astype(F32)
    out[kind.at_recv : kind.at_recv + 2, :] = recv[0, 0].astype(F32)
    for m in range(kind.sources):
        at = kind.at_layer + m
        out[at : at + 1, :] = layer_a[0, m].astype(F32)
        out[at + kind.sources : at + kind.sources + 1, :] = layer_b[0, m]
    if not kind.sources:
        row = layer_a[0, 0:1, :]
        live = lane < jnp.broadcast_to(layer_b[0:1, 0:1], (1, LANES))
        out[kind.at_layer : kind.at_layer + 1, :] = jnp.where(live, row, -1).astype(F32)
    size = kind.quads_pad
    if kind.table_turned:
        work[0 : kind.points, 0 : 3 * kind.quads] = table[...]
        turned = work[...]
        plain = jnp.transpose(turned)
    else:
        for a in range(3):
            work[a * size : a * size + kind.quads, 0 : kind.points] = table[
                a * kind.quads : (a + 1) * kind.quads, :
            ]
        plain = work[...]
        turned = jnp.transpose(plain)
    step = kind.points_pad
    high = high_part(plain)
    low = plain - high
    rows = high + pltpu.roll(low, step, 1) + pltpu.roll(high, 2 * step, 1)
    first[...] = rows[0 : 3 * size, 0 : kind.depth_in].astype(BF16)
    high = high_part(turned)
    low = turned - high
    wide = jnp.zeros((LANES, LANES), F32)
    high = jnp.concatenate([high, wide], axis=1)
    low = jnp.concatenate([low, wide], axis=1)
    rows = high + pltpu.roll(low, 3 * size, 1) + pltpu.roll(high, 6 * size, 1)
    second[...] = (-rows[0 : kind.points_pad, 0 : kind.depth_out]).astype(BF16)


def pack(kind, disp, vel, nodes, coefs, minv, send, recv, fill, layer_a, layer_b, table):
    def thin(array):
        return jnp.transpose(array, (0, 2, 1, 3))

    vmem = pl.BlockSpec(memory_space=pltpu.VMEM)
    hbm = pl.BlockSpec(memory_space=pl.ANY)
    if kind.sources:
        layer_a, layer_b = thin(layer_a), thin(layer_b)
    if kind.table_turned:
        table = table.T
    inputs = (
        thin(disp), thin(vel), thin(nodes), coefs, minv, send, recv, fill, layer_a, layer_b, table,
    )
    return pl.pallas_call(
        functools.partial(pack_kernel, kind),
        out_shape=[
            jax.ShapeDtypeStruct((kind.rows, LANES), F32),
            jax.ShapeDtypeStruct((3 * kind.quads_pad, kind.depth_in), BF16),
            jax.ShapeDtypeStruct((kind.points_pad, kind.depth_out), BF16),
        ],
        in_specs=[hbm] * len(inputs),
        out_specs=[vmem] * 3,
        scratch_shapes=[
            pltpu.VMEM((LANES, LANES), F32),
            *[pltpu.VMEM(array.shape, array.dtype) for array in inputs],
            pltpu.SemaphoreType.DMA((len(inputs),)),
        ],
        name="site_pack" if kind.sources else "reg_pack",
    )(*inputs)


def split_index(value):
    index = value.astype(jnp.int32)
    return index & (LANES - 1), index >> 7


def high_part(value):
    return value.astype(BF16).astype(F32)


def simulate(kind, width, unroll, own, mode, buf, lhs_in, lhs_out, layers, emit, begun, s):
    points, cuts, blocks = kind.points, kind.cuts, kind.blocks
    quads_pad = kind.quads_pad
    half_rows = 6 * blocks if kind.dense else 8 * kind.blocks_pad
    row8 = lax.broadcasted_iota(jnp.int32, (8, LANES), 0)
    low_half = row8 < 4
    row16 = lax.broadcasted_iota(jnp.int32, (16, LANES), 0)
    block_ids = [
        jnp.where(row16 < 8, 2 * j, 2 * j + 1).astype(F32).astype(BF16)
        for j in range(kind.blocks_pad // 2)
    ]
    zero16 = jnp.zeros((16, LANES), BF16)
    zero8 = jnp.zeros((8, LANES), F32)
    lane_ids = lax.broadcasted_iota(jnp.int32, (LANES, LANES), 1).astype(F32).astype(BF16)
    one = jnp.ones((LANES, LANES), BF16)
    none = jnp.zeros((LANES, LANES), BF16)
    main_rows = kind.tiles * 256

    def onehot(q, chunk_no, base_row, columns, at):
        if mode == "rest":
            return
        hit = columns[:, at : at + 1] == lane_ids
        tile, half, part = chunk_no // 4, (chunk_no // 2) % 2, chunk_no % 2
        rows = pl.ds(base_row + tile * 256 + part * LANES, LANES)
        s.onehot[q, half, rows, :] = jnp.where(hit, one, none)

    def hold_block(q, chunk_no, hi_row):
        s.block_of[q, chunk_no : chunk_no + 1, :] = hi_row.astype(F32)

    def columns_of(rows):
        if mode == "rest":
            return None
        count = rows.shape[0]
        if count < LANES:
            rows = jnp.concatenate([rows, jnp.zeros((LANES - count, LANES), F32)], axis=0)
        return jnp.transpose(rows).astype(BF16)

    def setup(q, _):
        for pair in range(6):
            for cut in range(cuts):
                at = kind.at_coefs + (pair * cuts + cut) * kind.quads
                lanes = slice(cut * LANES, (cut + 1) * LANES)
                if kind.quads_pad > kind.quads:
                    s.coefs[q, pair, :, lanes] = jnp.zeros((quads_pad, LANES), F32)
                s.coefs[q, pair, 0 : kind.quads, lanes] = buf[q, at : at + kind.quads, :]
        for cut in range(cuts):
            at = kind.at_nodes + cut * points
            value = buf[q, at : at + points, :]
            lo, hi = split_index(value)
            if kind.points_pad > points:
                s.lo[q, cut] = jnp.zeros((kind.points_pad, LANES), jnp.int32)
                s.hi[q, cut] = jnp.zeros((kind.points_pad, LANES), jnp.int32)
            s.lo[q, cut, 0:points, :] = lo
            s.hi[q, cut, 0:points, :] = hi
            columns = columns_of(lo.astype(F32))
            for p in range(points):
                onehot(q, cut * points + p, 0, columns, p)
                hold_block(q, cut * points + p, hi[p : p + 1, :])
        for chunk in range(kind.chunks, 4 * kind.tiles):
            columns = jnp.zeros((LANES, LANES), BF16)
            onehot(q, chunk, 0, columns, 0)
            hold_block(q, chunk, jnp.zeros((1, LANES), jnp.int32))
        extra = [buf[q, kind.at_recv : kind.at_recv + 2, :]]
        if kind.sources:
            extra.append(buf[q, kind.at_layer : kind.at_layer + kind.sources, :])
        extra.append(jnp.zeros((4 * kind.extra_tiles - kind.extra, LANES), F32))
        lo, hi = split_index(jnp.concatenate([e for e in extra if e.shape[0]], axis=0))
        columns = columns_of(lo.astype(F32))
        for chunk in range(4 * kind.extra_tiles):
            onehot(q, chunk, main_rows, columns, chunk)
            hold_block(q, 4 * kind.tiles + chunk, hi[chunk : chunk + 1, :])
        send_rows = [
            jnp.broadcast_to(buf[q, kind.at_send + side : kind.at_send + side + 1, :], (4, LANES))
            for side in range(2)
        ]
        s.send_lo[q], s.send_hi[q] = split_index(jnp.concatenate(send_rows, axis=0))
        if not kind.sources:
            row = buf[q, kind.at_layer : kind.at_layer + 1, :]
            s.layer_lo[q], s.layer_hi[q] = split_index(jnp.broadcast_to(row, (8, LANES)))
        for block in range(blocks):
            at = kind.at_disp + 3 * block
            now = buf[q, at : at + 3, :]
            at = kind.at_vel + 3 * block
            before = now - buf[q, at : at + 3, :]
            for ref, value in ((s.now, now), (s.before, before)):
                ref[q, block] = zero8
                ref[q, block, 0:3, :] = value
                ref[q, block, 4:7, :] = value
        return 0

    def setup_pair(pair, _):
        for k in range(2):
            setup(2 * pair + k, 0)
        return 0

    lax.fori_loop(0, width // 2, setup_pair, 0)
    for lane in range(unroll):
        s.parts[lane] = jnp.zeros(s.parts.shape[1:], F32)
        s.turn[lane] = jnp.zeros(s.turn.shape[1:], F32)
    s.sends[0] = zero8
    s.sends[width + 1] = zero8

    slabs = half_rows // 8
    slab_rows = [
        [divmod(8 * slab + row, blocks) for row in range(8)] for slab in range(slabs)
    ]
    slab_ids = {}
    for slab in range(slabs if kind.dense else 0):
        number = slab_rows[slab][0][1]
        if number not in slab_ids:
            slab_ids[number] = lax.rem(row8 + number, blocks).astype(F32)

    def dense_rows(q, chunk, rows):
        held = jnp.broadcast_to(s.block_of[q, chunk : chunk + 1, :], (8, LANES))
        hits = {number: held == ids for number, ids in slab_ids.items()}
        result = []
        for slab in range(slabs):
            places = slab_rows[slab]
            value = jnp.broadcast_to(rows[places[0][0]], (8, LANES))
            if places[7][0] != places[0][0]:
                other = jnp.broadcast_to(rows[places[7][0]], (8, LANES))
                value = jnp.where(row8 < places.index((places[7][0], 0)), value, other)
            result.append(jnp.where(hits[places[0][1]], value, 0.0))
        return result

    def dense_spread(q, first, values):
        parts = [dense_rows(q, first + number, rows) for number, rows in enumerate(values)]
        parts += [[zero8] * slabs] * (4 - len(values))
        columns = [
            jnp.concatenate(parts[k] + parts[k + 2], axis=0).astype(BF16) for k in range(2)
        ]
        return jnp.concatenate(columns, axis=1)

    def spread(q, first, values):
        blank = jnp.zeros((half_rows, LANES), BF16)
        parts = []
        for number, value8 in enumerate(values):
            doubled = jnp.concatenate([value8, value8], axis=0).astype(BF16)
            held = s.block_of[q, first + number : first + number + 1, :]
            held = jnp.broadcast_to(held, (16, LANES)).astype(BF16)
            parts.append(
                jnp.concatenate(
                    [jnp.where(held == ids, doubled, zero16) for ids in block_ids], axis=0
                )
            )
        parts += [blank] * (4 - len(values))
        return jnp.concatenate(
            [jnp.concatenate(parts[0:2], axis=1), jnp.concatenate(parts[2:4], axis=1)], axis=0
        )

    def scattered(q, first, rows_from, get, count):
        total = None
        for at in range(0, count, 4):
            build = dense_spread if kind.dense else spread
            left = build(q, first + at, [get(k) for k in range(at, min(at + 4, count))])
            rows = slice(rows_from + at * 64, rows_from + at * 64 + 256)
            right = jnp.concatenate([s.onehot[q, half, rows, :] for half in range(2)], axis=1)
            term = jnp.dot(left, right, preferred_element_type=F32)
            total = term if total is None else total + term
        return total

    def fold(total, lane):
        if kind.dense:
            value = total[0:half_rows, 0:LANES] + total[half_rows:, LANES:]
            for c in range(3):
                at = (c + 3) * blocks
                whole = value[c * blocks : (c + 1) * blocks, :] + value[at : at + blocks, :]
                for copy in (0, 4):
                    at = (c + copy) * kind.blocks_pad
                    s.turn[lane, at : at + blocks, :] = whole
            return [
                s.turn[lane, pl.ds(block, 8, stride=kind.blocks_pad), :]
                for block in range(blocks)
            ]
        folded = []
        for block in range(blocks):
            rows = slice(block * 8, block * 8 + 8)
            other = slice(half_rows + block * 8, half_rows + block * 8 + 8)
            value = total[rows, 0:LANES] + total[other, LANES : 2 * LANES]
            folded.append(value + pltpu.roll(value, 4, 0))
        return folded

    def choose(found, bits):
        for bit in bits:
            found = [
                jnp.where(bit, found[k + 1], found[k]) if k + 1 < len(found) else found[k]
                for k in range(0, len(found), 2)
            ]
        return found[0]

    def bits_of(hi):
        count = (blocks - 1).bit_length()
        return [(hi & (1 << k)) != 0 for k in range(count)]

    def lookup(row, lo):
        return jnp.take_along_axis(row, lo, axis=1, mode="promise_in_bounds")

    def pick(source, lo, hi):
        found = [lookup(source(block), lo) for block in range(blocks)]
        return jnp.where(hi < 0, 0.0, choose(found, bits_of(hi)))

    def force(q, lane):
        stacked = []
        picked = {}
        for cut in range(cuts):
            groups = {c: [] for c in range(3)}
            for at in range(0, kind.points_pad, 8):
                lo = s.lo[q, cut, at : at + 8, :]
                bits = bits_of(s.hi[q, cut, at : at + 8, :])
                for c in range(3):
                    found = [
                        lookup(jnp.broadcast_to(s.now[q, block, c : c + 1, :], (8, LANES)), lo)
                        for block in range(blocks)
                    ]
                    groups[c].append(choose(found, bits))
            for c in range(3):
                picked[c, cut] = jnp.concatenate(groups[c], axis=0)
        order = [(c, cut) for c in range(3) for cut in range(cuts)]
        for key in order:
            high = high_part(picked[key])
            rows = [high, high, picked[key] - high]
            pad = kind.depth_in - 3 * kind.points_pad
            if pad:
                rows.append(jnp.zeros((pad, LANES), F32))
            stacked.append(jnp.concatenate(rows, axis=0).astype(BF16))
        grad = jnp.dot(
            lhs_in[...], jnp.concatenate(stacked, axis=1), preferred_element_type=F32
        )
        stacked = []
        for number, (c, cut) in enumerate(order):
            lanes = slice(number * LANES, (number + 1) * LANES)
            cut_lanes = slice(cut * LANES, (cut + 1) * LANES)
            pieces = [grad[b * quads_pad : (b + 1) * quads_pad, lanes] for b in range(3)]
            coef = [s.coefs[q, pair, :, cut_lanes] for pair in range(6)]
            flux = jnp.concatenate(
                [
                    coef[PAIR_OF[a, 0]] * pieces[0]
                    + coef[PAIR_OF[a, 1]] * pieces[1]
                    + coef[PAIR_OF[a, 2]] * pieces[2]
                    for a in range(3)
                ],
                axis=0,
            )
            high = high_part(flux)
            rows = [high, high, flux - high]
            pad = kind.depth_out - 9 * quads_pad
            if pad:
                rows.append(jnp.zeros((pad, LANES), F32))
            stacked.append(jnp.concatenate(rows, axis=0).astype(BF16))
        elem = jnp.dot(
            lhs_out[...], jnp.concatenate(stacked, axis=1), preferred_element_type=F32
        )
        for number, (c, cut) in enumerate(order):
            value = elem[:, number * LANES : (number + 1) * LANES]
            high = high_part(value)
            size = kind.points_pad
            s.parts[lane, cut, c * size : (c + 1) * size, :] = high
            at = (c + (3 if kind.dense else 4)) * size
            s.parts[lane, cut, at : at + size, :] = value - high
        def entry(chunk):
            cut, p = divmod(chunk, points)
            if kind.dense:
                rows = [part * kind.points_pad + p for part in range(6)]
                return [s.parts[lane, cut, row : row + 1, :] for row in rows]
            return s.parts[lane, cut, pl.ds(p, 8, stride=kind.points_pad), :]

        total = scattered(q, 0, 0, entry, kind.chunks)
        folded = fold(total, lane)
        for block in range(blocks):
            s.force[q, block] = folded[block]
        s.sends[q + 1] = pick(lambda block: folded[block], s.send_lo[q], s.send_hi[q])

    def split8(value):
        high = high_part(value)
        if kind.dense:
            return [part[c : c + 1, :] for part in (high, value - high) for c in range(3)]
        return jnp.where(low_half, high, value - high)

    def update(q, lane, step, forces, sends):
        lower = sends[q]
        upper = sends[q + 2]
        values = [
            jnp.where(low_half, pltpu.roll(lower, 4, 0), lower),
            jnp.where(low_half, upper, pltpu.roll(upper, 4, 0)),
        ]
        for m in range(kind.sources):
            at = kind.at_layer + kind.sources + m
            rows = [layers[m][step, c, pl.ds(q, 1), :] for c in range(3)]
            rows = jnp.concatenate([*rows, jnp.zeros((1, LANES), F32)] * 2, axis=0)
            values.append(rows * buf[q, at : at + 1, :])
        total = scattered(
            q, 4 * kind.tiles, main_rows, lambda k: split8(values[k]), len(values)
        )
        folded = fold(total, lane)
        after = []
        for block in range(blocks):
            now = s.now[q, block]
            scale = buf[q, kind.at_minv + block : kind.at_minv + block + 1, :]
            whole = forces[q, block] + folded[block]
            value = 2.0 * now - s.before[q, block] + scale * whole
            s.before[q, block] = now
            s.now[q, block] = value
            after.append(value)
        if emit is not None:
            picked = pick(lambda block: after[block], s.layer_lo[q], s.layer_hi[q])
            for c in range(3):
                emit[step, c, pl.ds(q, 1), :] = picked[c : c + 1, :]

    def all_forces():
        def forces(group, _):
            for lane in range(unroll):
                force(group * unroll + lane, lane)
            return 0

        lax.fori_loop(0, width // unroll, forces, 0)

    def all_updates(step, forces, sends):
        def updates(group, _):
            for lane in range(unroll):
                update(group * unroll + lane, lane, step, forces, sends)
            return 0

        lax.fori_loop(0, width // unroll, updates, 0)

    def one_step(step, _):
        all_forces()
        all_updates(step, s.force, s.sends)
        return 0

    if mode == "first":
        all_forces()
        begun[0][...] = s.force[...]
        begun[1][...] = s.sends[...]
        return
    done = 0
    if mode == "rest":
        all_updates(0, *begun)
        done = 1
    tail = max(done, STEPS - 2)
    lax.fori_loop(done, tail, one_step, 0)
    for step in range(tail, STEPS):
        reach = STEPS - step
        for span, run in (
            (min(2 * reach + 1, width), force),
            (min(2 * reach - 1, width), functools.partial(update, step=step, forces=s.force, sends=s.sends)),
        ):
            first = jnp.clip(own - span // 2, 0, width - span)
            for lane in range(span):
                run(first + lane, lane % unroll)


SCRATCH = (
    "onehot", "block_of", "coefs", "lo", "hi", "send_lo", "send_hi", "layer_lo", "layer_hi",
    "now", "before", "force", "sends", "parts", "turn",
)


def scratch_of(kind, width, unroll):
    tiles = kind.tiles + kind.extra_tiles
    return [
        pltpu.VMEM(onehot_shape(kind, width), BF16),
        pltpu.VMEM((width, 4 * tiles, LANES), F32),
        pltpu.VMEM((width, 6, kind.quads_pad, kind.elems), F32),
        pltpu.VMEM((width, kind.cuts, kind.points_pad, LANES), jnp.int32),
        pltpu.VMEM((width, kind.cuts, kind.points_pad, LANES), jnp.int32),
        pltpu.VMEM((width, 8, LANES), jnp.int32),
        pltpu.VMEM((width, 8, LANES), jnp.int32),
        pltpu.VMEM((width, 8, LANES), jnp.int32),
        pltpu.VMEM((width, 8, LANES), jnp.int32),
        pltpu.VMEM((width, kind.blocks, 8, LANES), F32),
        pltpu.VMEM((width, kind.blocks, 8, LANES), F32),
        pltpu.VMEM((width, kind.blocks, 8, LANES), F32),
        pltpu.VMEM((width + 2, 8, LANES), F32),
        pltpu.VMEM((unroll, kind.cuts, 8 * kind.points_pad, LANES), F32),
        pltpu.VMEM((unroll, 8 * kind.blocks_pad, LANES), F32),
    ]


class Refs:
    pass


def window_base(index, count, width):
    return jnp.clip(index - STEPS, 0, count - width)


def sim_kernel(kind, width, unroll, offsets, mode, spare, *refs):
    sub = lax.axis_index("sub")
    count = lax.axis_size("sub")
    chips = count // 2
    bufs, refs = refs[:2], refs[2:]
    lhs_in, lhs_out, refs = refs[0], refs[1], refs[2:]
    layers = begun = emit = final = None
    if mode == "rest":
        layers, refs = refs[: kind.sources], refs[kind.sources :]
        begun, refs = refs[:3], refs[3:]
    if mode == "first":
        begun, refs = refs[:3], refs[3:]
    else:
        final, refs = refs[0], refs[1:]
    if mode == "all":
        emit, refs = refs[0], refs[1:]
    refs = refs[spare:]
    buf, sem, refs = refs[0], refs[1], refs[2:]
    s = Refs()
    if mode != "all":
        s.onehot, begun = begun[2], begun[:2]
    for name, ref in zip(SCRATCH[mode != "all" :], refs, strict=True):
        setattr(s, name, ref)
    base = window_base(sub, count, width)
    if width < count:
        buf[...] = jnp.zeros(buf.shape, F32)
    copies = []
    for number, offset in enumerate(offsets):
        for other in range(2):
            chip = lax.rem(sub // 2 - offset + chips, chips)
            core = lax.rem(sub, 2)
            slot = chip * 2 + (core if other == 0 else 1 - core) - base
            at = 2 * number + other
            inside = jnp.logical_and(slot >= 0, slot < width)
            slot = jnp.clip(slot, 0, width - 1)
            copy = pltpu.make_async_copy(bufs[other].at[number], buf.at[slot], sem.at[at])
            copies.append((inside, copy))
    for phase in ("start", "wait"):
        for inside, copy in copies:
            if width < count:
                pl.when(inside)(getattr(copy, phase))
            else:
                getattr(copy, phase)()
    simulate(
        kind, width, unroll, sub - base, mode, buf, lhs_in, lhs_out, layers, emit, begun, s
    )
    if final is None:
        return
    for block in range(kind.blocks):
        for c in range(3):
            final[0, c, :, block * LANES : (block + 1) * LANES] = s.now[
                sub - base, block, c : c + 1, :
            ]


def onehot_shape(kind, width):
    return (width, 2, (kind.tiles + kind.extra_tiles) * 256, LANES)


def begun_shapes(kind, width):
    return [
        jax.ShapeDtypeStruct((width, kind.blocks, 8, LANES), F32),
        jax.ShapeDtypeStruct((width + 2, 8, LANES), F32),
        jax.ShapeDtypeStruct(onehot_shape(kind, width), BF16),
    ]


def vmem_limit(width):
    return (24 if width <= 8 else 60) * 1024 * 1024


def layer_shape(width):
    return jax.ShapeDtypeStruct((STEPS, 3, width, LANES), F32)


def run_sim(kind, width, unroll, offsets, mode, bufs, tables, more, spare):
    if mode == "first":
        out_shape = begun_shapes(kind, width)
    else:
        out_shape = [jax.ShapeDtypeStruct((1, 3, 1, kind.count), F32)]
    if mode == "all":
        out_shape.append(layer_shape(width))
    vmem = pl.BlockSpec(memory_space=pltpu.VMEM)
    hbm = pl.BlockSpec(memory_space=pl.ANY)
    return pl.pallas_call(
        functools.partial(sim_kernel, kind, width, unroll, offsets, mode, len(spare)),
        out_shape=out_shape + spare,
        in_specs=[hbm] * len(bufs) + [vmem] * (2 + len(more)),
        out_specs=[vmem] * len(out_shape) + [hbm] * len(spare),
        scratch_shapes=[
            pltpu.VMEM((width, kind.rows, LANES), F32),
            pltpu.SemaphoreType.DMA((2 * len(offsets),)),
        ]
        + scratch_of(kind, width, unroll)[mode != "all" :],
        compiler_params=pltpu.CompilerParams(vmem_limit_bytes=vmem_limit(width)),
        name="sim_" + mode,
    )(*bufs, *tables, *more)


def blank_kernel(final, *rest):
    final[...] = jnp.zeros(final.shape, F32)


def gather_window(value, groups, offsets, count):
    chips = count // 2
    low, high = groups

    def moved(array, chip_shift, flip):
        route = []
        for grp in range(low, high):
            for index in range(count):
                chip, core = divmod(index, 2)
                target = ((chip + chip_shift) % chips) * 2 + (core ^ flip)
                route.append((grp * count + index, grp * count + target))
        return lax.ppermute(array, ("grp", "sub"), route)

    if len(offsets) == 1:
        joined = value[None]
        return [joined, moved(joined, 0, 1)]
    by_chip = [value if shift % chips == 0 else moved(value, shift, 0) for shift in offsets]
    joined = pl.pallas_call(
        join_kernel,
        out_shape=jax.ShapeDtypeStruct((len(offsets), *value.shape), F32),
        in_specs=[pl.BlockSpec(memory_space=pltpu.VMEM)] * len(offsets),
        out_specs=pl.BlockSpec(memory_space=pltpu.VMEM),
        name="join",
    )(*by_chip)
    return [joined, moved(joined, 0, 1)]


def join_kernel(*refs):
    for number, ref in enumerate(refs[:-1]):
        refs[-1][number] = ref[...]


def shards(
    reg_disp, reg_vel, site_disp, site_vel, reg_nodes, site_nodes, reg_coefs, site_coefs,
    reg_table, site_table, reg_minv, site_minv, reg_send, reg_recv, site_send, site_recv,
    slot_fill, layer_src, layer_fill, layer_dst, layer_stiff,
):
    group_count = lax.axis_size("grp")
    count = lax.axis_size("sub")
    site_groups = group_count // 4
    reg_groups = 3 * site_groups
    reg = Kind(reg_nodes, reg_coefs, reg_disp, 0)
    site = Kind(site_nodes, site_coefs, site_disp, 3)
    unroll = min(UNROLL, count)
    width = min(count, up_to(2 * STEPS + 1, unroll))
    chips = count // 2
    reach = STEPS // 2
    if 2 * reach + 1 >= chips:
        offsets = tuple(range(chips))
    else:
        offsets = tuple(range(-reach, reach + 1))
    is_site = lax.axis_index("grp") >= reg_groups
    vmem = pl.BlockSpec(memory_space=pltpu.VMEM)
    hbm = pl.BlockSpec(memory_space=pl.ANY)
    site_spare = [jax.ShapeDtypeStruct((len(offsets), site.rows, LANES), F32)] * 2 + [
        jax.ShapeDtypeStruct((3 * site.quads_pad, site.depth_in), BF16),
        jax.ShapeDtypeStruct((site.points_pad, site.depth_out), BF16),
        *begun_shapes(site, width),
    ]

    def regional():
        buf, *tables = pack(
            reg, reg_disp, reg_vel, reg_nodes, reg_coefs, reg_minv, reg_send, reg_recv,
            slot_fill, layer_src, layer_fill, reg_table,
        )
        bufs = gather_window(buf, (0, reg_groups), offsets, count)
        final, layer, *spare = run_sim(
            reg, width, unroll, offsets, "all", bufs, tables, (), site_spare
        )
        return (final, layer, *spare)

    def prepare_site():
        buf, *tables = pack(
            site, site_disp, site_vel, site_nodes, site_coefs, site_minv, site_send, site_recv,
            slot_fill, layer_dst, layer_stiff, site_table,
        )
        bufs = gather_window(buf, (reg_groups, group_count), offsets, count)
        final, layer = pl.pallas_call(
            blank_kernel,
            out_shape=[
                jax.ShapeDtypeStruct((1, 3, 1, reg.count), F32),
                layer_shape(width),
            ],
            out_specs=[vmem, hbm],
            name="blank",
        )()
        begun = run_sim(site, width, unroll, offsets, "first", bufs, tables, (), [])
        return (final, layer, *bufs, *tables, *begun)

    reg_final, layer_out, *rest = lax.cond(is_site, prepare_site, regional)
    site_bufs, site_tables, begun = rest[:2], rest[2:4], rest[4:]
    layers = [
        lax.ppermute(
            layer_out,
            "grp",
            [(m * site_groups + i, reg_groups + i) for i in range(site_groups)],
        )
        for m in range(3)
    ]

    def run_site():
        more = (*layers, *begun)
        return run_sim(site, width, unroll, offsets, "rest", site_bufs, site_tables, more, [])[0]

    def no_site():
        return jnp.zeros((1, 3, 1, site.count), F32)

    site_final = lax.cond(is_site, run_site, no_site)
    return jnp.transpose(reg_final, (0, 2, 1, 3)), jnp.transpose(site_final, (0, 2, 1, 3))


def solution(mesh):
    def spec(rank):
        return P("grp", "sub", *([None] * (rank - 2)))

    ranks = (4, 4, 4, 4, 4, 4, 6, 6, 0, 0, 3, 3, 4, 4, 4, 4, 3, 3, 2, 4, 4)
    return jax.shard_map(
        shards,
        mesh=mesh,
        in_specs=tuple(spec(rank) if rank else P() for rank in ranks),
        out_specs=(spec(4), spec(4)),
        check_vma=False,
    )
```
